8 devices in a mesh: fsdp: 8 (over z, y, x, core).
Axes of the slice: x: 2, y: 2, z: 1, core: 2. Of those that a mesh axis runs over, the one named last changes fastest.
Arguments:
- w_up: bfloat16 [1, 2048, 5632], P(None, 'fsdp')
- w_down: bfloat16 [1, 5632, 2048], P(None, 'fsdp')
- tokens_in: bfloat16 [3, 4096, 2048], P(None, 'fsdp')
- cotangent: bfloat16 [3, 4096, 2048], P(None, 'fsdp')
Outputs:
- output 1: bfloat16 [3, 4096, 2048], P(None, 'fsdp')
- output 2: float32 [1, 2048, 5632], P(None, 'fsdp')
- output 3: float32 [1, 5632, 2048], P(None, 'fsdp')
All inputs are finite; a program needn't handle non-finite values.
Results may differ from the reference program's by a relative error of at most 0.001.
Values are sent between devices in bfloat16 or wider.
A program may use at most 1 GiB of HBM per device.

```python
import jax
import jax.numpy as jnp
from jax import lax

D_MODEL = 2048
D_FF = 5632
LAYERS = 1
MICROBATCHES = 3
TOK_DEV = 512
GROUP_SIZE = 8

TOK_ALL = GROUP_SIZE * TOK_DEV


def setup_inputs(seed: int = 0) -> dict:
    base_key = jax.random.key(seed)
    key_up, key_down, key_tok, key_cot = jax.random.split(base_key, 4)
    w_up = (jax.random.normal(key_up, (LAYERS, D_MODEL, D_FF), jnp.float32) * D_MODEL ** -0.5).astype(jnp.bfloat16)
    w_down = (jax.random.normal(key_down, (LAYERS, D_FF, D_MODEL), jnp.float32) * D_FF ** -0.5).astype(jnp.bfloat16)
    tokens_in = jax.random.normal(key_tok, (MICROBATCHES, TOK_ALL, D_MODEL), jnp.float32).astype(jnp.bfloat16)
    cot_scale = (MICROBATCHES * TOK_ALL) ** -0.5
    cotangent = (jax.random.normal(key_cot, (MICROBATCHES, TOK_ALL, D_MODEL), jnp.float32) * cot_scale).astype(jnp.bfloat16)
    return {'w_up': w_up, 'w_down': w_down, 'tokens_in': tokens_in, 'cotangent': cotangent}


def gelu_fn(pre_act):
    return jax.nn.gelu(pre_act, approximate=True)


def layer_forward(rows_in, up_mat, down_mat):
    pre_act = jnp.dot(rows_in, up_mat, preferred_element_type=jnp.float32).astype(jnp.bfloat16)
    hidden = gelu_fn(pre_act.astype(jnp.float32)).astype(jnp.bfloat16)
    summed = rows_in.astype(jnp.float32) + jnp.dot(hidden, down_mat, preferred_element_type=jnp.float32)
    return summed.astype(jnp.bfloat16)


def layer_backward(rows_in, up_mat, down_mat, grad_rows):
    pre_f32 = jnp.dot(rows_in, up_mat, preferred_element_type=jnp.float32).astype(jnp.bfloat16).astype(jnp.float32)
    hidden_f32, pull_back = jax.vjp(gelu_fn, pre_f32)
    hidden = hidden_f32.astype(jnp.bfloat16)
    grad_down = jnp.dot(hidden.T, grad_rows, preferred_element_type=jnp.float32)
    grad_hid = jnp.dot(grad_rows, down_mat.T, preferred_element_type=jnp.float32)
    grad_pre = pull_back(grad_hid)[0].astype(jnp.bfloat16)
    grad_up = jnp.dot(rows_in.T, grad_pre, preferred_element_type=jnp.float32)
    grad_prev = grad_rows.astype(jnp.float32) + jnp.dot(grad_pre, up_mat.T, preferred_element_type=jnp.float32)
    return grad_prev.astype(jnp.bfloat16), grad_up, grad_down


def reference(w_up, w_down, tokens_in, cotangent):
    def micro_step(acc_pair, micro_in):
        rows_in, cot_rows = micro_in

        def fwd_step(rows_cur, mat_pair):
            return layer_forward(rows_cur, mat_pair[0], mat_pair[1]), rows_cur

        rows_out, saved_rows = lax.scan(fwd_step, rows_in, (w_up, w_down))

        def bwd_step(grad_rows, layer_items):
            grad_prev, grad_up, grad_down = layer_backward(layer_items[0], layer_items[1], layer_items[2], grad_rows)
            return grad_prev, (grad_up, grad_down)

        _, grad_pair = lax.scan(bwd_step, cot_rows, (saved_rows, w_up, w_down), reverse=True)
        return (acc_pair[0] + grad_pair[0], acc_pair[1] + grad_pair[1]), rows_out

    acc_init = (jnp.zeros(w_up.shape, jnp.float32), jnp.zeros(w_down.shape, jnp.float32))
    acc_pair, tokens_out = lax.scan(micro_step, acc_init, (tokens_in, cotangent))
    return tokens_out, acc_pair[0], acc_pair[1]
```

```python
import functools
import math

import jax
import jax.numpy as jnp
from jax import lax
from jax.experimental import pallas as pl
from jax.experimental.pallas import tpu as pltpu
from jax.sharding import PartitionSpec as P

F32 = jnp.float32
BF16 = jnp.bfloat16
N_CHUNK = 11
LAG_T = 4
LAG_Z = 8
N_K = 8
N_H = 3
N_T = 4
Y_STEP = 5
GELU_C = math.sqrt(2.0 / math.pi)
NN = (((1,), (0,)), ((), ()))
NT_DIMS = (((1,), (1,)), ((), ()))
TN_DIMS = (((0,), (0,)), ((), ()))


def matmul(a, b, dims=NN):
    return lax.dot_general(a, b, dims, preferred_element_type=F32)


def aligned(start, size):
    return pl.ds(pl.multiple_of(start, size), size)


def kernel(sizes, w1, w2, x, g, y, gup, gdown, w1f, w2f, a_h, h_h, ht_h, r_s, r_h, r_t,
           x_v, g_v, y_acc, w1_ss, w1_rs, w2_ss, w2_rs, c_rs, s_ss, h_ss, t_ss, loc, out_sem, io_sem, ld_sem):
    tokens, d_model, d_ff = sizes
    fc = d_ff // N_CHUNK
    d_blk = d_model // 8
    f_blk = d_ff // 8
    r2 = f_blk // N_CHUNK
    n_tile = d_model // fc
    n_q = 2 * N_CHUNK
    row_t = tokens // 3
    n_row = 3
    pieces = ((0, 2), (2, 3), (5, 3), (8, 3))
    n_piece = 4
    p_rows = f_blk // n_piece

    me = lax.axis_index('fsdp')
    core = me % 2
    cx = (me // 2) % 2
    cy = me // 4
    chip = me // 2

    def dev(flip_y, flip_x, flip_c):
        yy = 1 - cy if flip_y else cy
        xx = 1 - cx if flip_x else cx
        cc = 1 - core if flip_c else core
        return 4 * yy + 2 * xx + cc

    sib, xn, yn = dev(0, 0, 1), dev(0, 1, 0), dev(1, 0, 0)
    diag = dev(1, 1, 0)
    origins = (xn, yn, diag, sib, dev(0, 1, 1), dev(1, 0, 1), dev(1, 1, 1))

    def remote(src, dst, ssem, rsem, to):
        return pltpu.make_async_remote_copy(src_ref=src, dst_ref=dst, send_sem=ssem, recv_sem=rsem,
                                            device_id=(to,), device_id_type=pl.DeviceIdType.MESH)

    barrier = pltpu.get_barrier_semaphore()
    for other in (sib, xn, yn):
        pl.semaphore_signal(barrier, inc=1, device_id=(other,), device_id_type=pl.DeviceIdType.MESH)
    pl.semaphore_wait(barrier, 3)

    def w1_cols(p):
        return pl.ds(pieces[p][0] * fc, pieces[p][1] * fc)

    def w1_copy(kind, p, origin, to, own=False):
        src = w1.at[:, w1_cols(p)] if own else w1f.at[origin, :, w1_cols(p)]
        return remote(src, w1f.at[origin, :, w1_cols(p)], w1_ss.at[kind, p], w1_rs.at[kind, p], to)

    def w2_copy(kind, p, origin, to, own=False):
        rows = aligned(p * p_rows, p_rows)
        full = aligned(origin * f_blk + p * p_rows, p_rows)
        src = w2.at[rows, :] if own else w2f.at[full, :]
        return remote(src, w2f.at[full, :], w2_ss.at[kind, p], w2_rs.at[kind, p], to)

    def w1_recv(kind, p):
        w1_copy(kind, p, origins[kind], me).wait_recv()

    def w2_recv(kind, p):
        w2_copy(kind, p, origins[kind], me).wait_recv()

    def own_w1(p):
        w1_copy(0, p, me, xn, own=True).start()
        w1_copy(1, p, me, yn, own=True).start()

    def own_w2(p):
        w2_copy(0, p, me, xn, own=True).start()
        w2_copy(1, p, me, yn, own=True).start()

    own_w1(0)
    own_w1(1)
    for p in range(n_piece):
        w1_copy(3, p, me, sib, own=True).start()
    for p in range(n_piece):
        w2_copy(3, p, me, sib, own=True).start()

    load_x = pltpu.make_async_copy(x, x_v, io_sem.at[0])
    load_g = pltpu.make_async_copy(g, g_v, io_sem.at[1])
    load_x.start()
    load_g.start()

    def stage_own(buf1, buf2):
        in1 = pltpu.make_async_copy(w1, buf1, io_sem.at[2])
        in2 = pltpu.make_async_copy(w2, buf2, io_sem.at[3])
        in1.start()
        in2.start()
        in1.wait()
        out1 = pltpu.make_async_copy(buf1, w1f.at[me], io_sem.at[2])
        out1.start()
        in2.wait()
        out2 = pltpu.make_async_copy(buf2, w2f.at[aligned(me * f_blk, f_blk), :], io_sem.at[3])
        out2.start()
        out1.wait()
        out2.wait()

    pl.run_scoped(stage_own, pltpu.VMEM((d_blk, d_ff), BF16), pltpu.VMEM((f_blk, d_model), BF16))
    load_x.wait()
    load_g.wait()

    def init_rows(r, _):
        rows = aligned(r * row_t, row_t)
        y_acc[rows, :] = x_v[rows, :].astype(F32)
        return 0

    lax.fori_loop(0, n_row, init_rows, 0)

    def pass_one(wb, ab, hb, htb):
        def w1_load(k, slot):
            return pltpu.make_async_copy(w1f.at[:, :, aligned(k * fc, fc)], wb.at[slot], ld_sem.at[slot])

        def stores(k, slot):
            cols = aligned(k * fc, fc)
            return (pltpu.make_async_copy(ab.at[slot], a_h.at[:, cols], loc.at[0, slot]),
                    pltpu.make_async_copy(hb.at[slot], h_h.at[:, cols], loc.at[1, slot]),
                    pltpu.make_async_copy(htb.at[slot], ht_h.at[cols, :], loc.at[2, slot]))

        def compute(p):
            for kind in (3, 4, 5, 6):
                w1_recv(kind, p)
            first, count = pieces[p]
            w1_load(first, first % 2).start()

            def chunk(k, _):
                slot = k % 2
                w1_load(k, slot).wait()

                @pl.when(k + 1 < first + count)
                def _():
                    w1_load(k + 1, 1 - slot).start()

                @pl.when(k >= 2)
                def _():
                    for cp in stores(k - 2, slot):
                        cp.wait()

                def rows_loop(r, _):
                    rows = aligned(r * row_t, row_t)
                    acc = matmul(x_v[rows, :], wb[slot].reshape(d_model, fc)).astype(BF16)
                    ab[slot, rows, :] = acc
                    u = acc.astype(F32)
                    t = jnp.tanh(GELU_C * (u + 0.044715 * (u * u * u)))
                    hid = (u * (0.5 * (1.0 + t))).astype(BF16)
                    hb[slot, rows, :] = hid
                    htb[slot, :, rows] = hid.T
                    return 0

                lax.fori_loop(0, n_row, rows_loop, 0)
                for cp in stores(k, slot):
                    cp.start()
                return 0

            lax.fori_loop(first, first + count, chunk, 0)

        def diag_forward(p):
            w1_recv(2, p)
            w1_copy(6, p, diag, sib).start()

        for p in range(n_piece):
            w1_recv(0, p)
            w1_copy(4, p, xn, sib).start()
            if p % 2:
                w1_copy(2, p, xn, yn).start()
            w1_recv(1, p)
            w1_copy(5, p, yn, sib).start()
            if not p % 2:
                w1_copy(2, p, yn, xn).start()
            if p + 2 < n_piece:
                own_w1(p + 2)
            else:
                own_w2(p + 2 - n_piece)
            if p >= 1:
                diag_forward(p - 1)
            if p >= 2:
                compute(p - 2)
        own_w2(2)
        own_w2(3)
        diag_forward(n_piece - 1)
        compute(n_piece - 2)
        compute(n_piece - 1)
        for k in (N_CHUNK - 2, N_CHUNK - 1):
            for cp in stores(k, k % 2):
                cp.wait()

    pl.run_scoped(pass_one, pltpu.VMEM((2, 8, d_blk, fc), BF16), pltpu.VMEM((2, tokens, fc), BF16),
                  pltpu.VMEM((2, tokens, fc), BF16), pltpu.VMEM((2, fc, tokens), BF16))

    def pick(par, even, odd):
        return even * (1 - par) + odd * par

    def first_dev(q):
        return pick(q % 2, xn, yn)

    def second_dev(q):
        return pick(q % 2, yn, xn)

    def chips_of(q):
        return (first_dev(q) // 2, 3 - chip, chip, second_dev(q) // 2)

    def main(s_b, m_b, k_b, h_b, t_b, z_b, st_s, st_h, st_t, q_v, lhs, w2e, a_v, w2y, hy):

        def send_s(q):
            return remote(s_b.at[q % 2], r_s.at[q], s_ss.at[q % 2], c_rs.at[0, q], sib)

        def send_h(q):
            return remote(h_b.at[q % N_H], r_h.at[q], h_ss.at[q % N_H], c_rs.at[1, q], first_dev(q))

        def send_t(q):
            return remote(t_b.at[q % N_T], r_t.at[q], t_ss.at[q % N_T], c_rs.at[2, q], second_dev(q))

        def lhs_loads(q):
            cps = []
            for b, mb in enumerate(chips_of(q)):
                for j, cc in enumerate((1 - core, core)):
                    rows = aligned(f_blk * (2 * mb + cc) + r2 * q, r2)
                    cps.append(pltpu.make_async_copy(ht_h.at[rows, :], lhs.at[4 * j + b], ld_sem.at[0]))
            return cps

        def lhs_wait():
            pltpu.make_async_copy(lhs, lhs, ld_sem.at[0]).wait()

        def e_loads(k):
            return (pltpu.make_async_copy(w2f.at[aligned(k * fc, fc), :], w2e, ld_sem.at[1]),
                    pltpu.make_async_copy(a_h.at[:, aligned(k * fc, fc)], a_v, ld_sem.at[2]))

        def y_loads(k):
            return (pltpu.make_async_copy(w2f.at[aligned(k * fc, fc), :], w2y, ld_sem.at[3]),
                    pltpu.make_async_copy(h_h.at[:, aligned(k * fc, fc)], hy, ld_sem.at[4]))

        def z_out(q, cond_down):
            slot = q % 2
            if cond_down:
                return [pltpu.make_async_copy(z_b.at[slot, n * r2:(n + 1) * r2, :],
                                              gdown.at[aligned(q * r2, r2), n * fc:(n + 1) * fc], out_sem.at[slot])
                        for n in range(n_tile)]
            return [pltpu.make_async_copy(z_b.at[slot], gup.at[:, aligned((q - N_CHUNK) * fc, fc)], out_sem.at[slot])]

        def z_wait(q):
            pltpu.make_async_copy(z_b.at[q % 2], gup.at[:, pl.ds(0, fc)], out_sem.at[q % 2]).wait()

        for cp in lhs_loads(0):
            cp.start()

        def step(s, _):
            @pl.when(s < n_piece)
            def _():
                w2_recv(0, s)
                w2_copy(4, s, xn, sib).start()
                w2_recv(1, s)
                w2_copy(5, s, yn, sib).start()
                w2_copy(2, s, pick(s % 2, yn, xn), pick(s % 2, xn, yn)).start()

            @pl.when((s >= 1) & (s < n_piece + 1))
            def _():
                w2_recv(2, s - 1)
                w2_copy(6, s - 1, diag, sib).start()

            @pl.when(s == Y_STEP)
            def _():
                for p in range(n_piece):
                    for kind in (3, 4, 5, 6):
                        w2_recv(kind, p)
                for cp in y_loads(0):
                    cp.start()
                for cp in e_loads(0):
                    cp.start()

            @pl.when((s >= 1) & (s - 1 < n_q))
            def _():
                q = s - 1
                send_s(q).wait_recv()
                ld = pltpu.make_async_copy(r_s.at[q], st_s, io_sem.at[0])
                ld.start()

                @pl.when(q >= N_H)
                def _():
                    send_h(q - N_H).wait_send()

                ld.wait()
                h_b[q % N_H] = m_b[0:2] + st_s[0:2]
                k_b[q % N_K] = m_b[2:4] + st_s[2:4]
                send_h(q).start()

            @pl.when((s >= LAG_T) & (s - LAG_T < n_q))
            def _():
                q = s - LAG_T
                send_h(q).wait_recv()
                ld = pltpu.make_async_copy(r_h.at[q], st_h, io_sem.at[1])
                ld.start()

                @pl.when(q >= N_T)
                def _():
                    send_t(q - N_T).wait_send()

                ld.wait()
                t_b[q % N_T] = k_b[q % N_K, 1] + st_h[1]
                send_t(q).start()
                k_b[q % N_K, 0] = k_b[q % N_K, 0] + st_h[0]

            @pl.when(s >= LAG_Z)
            def _():
                q = s - LAG_Z
                send_t(q).wait_recv()
                ld = pltpu.make_async_copy(r_t.at[q], st_t, io_sem.at[2])
                ld.start()

                @pl.when(q >= 2)
                def _():
                    z_wait(q - 2)

                ld.wait()
                z_b[q % 2] = k_b[q % N_K, 0] + st_t[...]

                @pl.when(q < N_CHUNK)
                def _():
                    for cp in z_out(q, True):
                        cp.start()

                @pl.when(q >= N_CHUNK)
                def _():
                    for cp in z_out(q, False):
                        cp.start()

            @pl.when((s >= 2) & (s < n_q))
            def _():
                send_s(s - 2).wait_send()

            @pl.when(s < N_CHUNK)
            def _():
                lhs_wait()

                def tile(n, _):
                    cols = aligned(n * fc, fc)
                    res = matmul(lhs[...].reshape(8 * r2, tokens), g_v[:, cols])
                    rows = aligned(n * r2, r2)
                    for b in range(4):
                        s_b[s % 2, b, rows, :] = res[b * r2:(b + 1) * r2]
                        m_b[b, rows, :] = res[(4 + b) * r2:(5 + b) * r2]
                    return 0

                lax.fori_loop(0, n_tile, tile, 0)
                send_s(s).start()

                @pl.when(s + 1 < N_CHUNK)
                def _():
                    for cp in lhs_loads(s + 1):
                        cp.start()

            @pl.when((s >= N_CHUNK) & (s < n_q))
            def _():
                k = s - N_CHUNK
                for cp in e_loads(k):
                    cp.wait()

                def rows_loop(r, _):
                    rows = aligned(r * row_t, row_t)
                    e = matmul(g_v[rows, :], w2e[...], NT_DIMS)
                    u = a_v[rows, :].astype(F32)
                    u2 = u * u
                    t = jnp.tanh(GELU_C * (u + 0.044715 * (u2 * u)))
                    slope = 0.5 * (1.0 + t) + (0.5 * u * (1.0 - t * t)) * GELU_C * (1.0 + 0.134145 * u2)
                    q_v[rows, :] = (e * slope).astype(BF16)
                    return 0

                lax.fori_loop(0, n_row, rows_loop, 0)

                @pl.when(k + 1 < N_CHUNK)
                def _():
                    for cp in e_loads(k + 1):
                        cp.start()

                for b, mb in enumerate(chips_of(s)):
                    for cc, dst in ((1 - core, s_b.at[s % 2]), (core, m_b)):
                        rows = aligned(d_blk * (2 * mb + cc), d_blk)
                        dst[b] = matmul(x_v[:, rows], q_v[...], TN_DIMS)
                send_s(s).start()

            @pl.when((s >= Y_STEP) & (s < Y_STEP + N_CHUNK))
            def _():
                k = s - Y_STEP
                for cp in y_loads(k):
                    cp.wait()

                def rows_loop(r, _):
                    rows = aligned(r * row_t, row_t)
                    y_acc[rows, :] += matmul(hy[rows, :], w2y[...])
                    return 0

                lax.fori_loop(0, n_row, rows_loop, 0)

                @pl.when(k + 1 < N_CHUNK)
                def _():
                    for cp in y_loads(k + 1):
                        cp.start()

            @pl.when(s == Y_STEP + N_CHUNK)
            def _():
                for n in range(n_tile):
                    hy[...] = y_acc[:, n * fc:(n + 1) * fc].astype(BF16)
                    cp = pltpu.make_async_copy(hy, y.at[:, n * fc:(n + 1) * fc], ld_sem.at[4])
                    cp.start()
                    cp.wait()

            return 0

        lax.fori_loop(0, n_q + LAG_Z, step, 0)
        send_s(n_q - 2).wait_send()
        send_s(n_q - 1).wait_send()
        for q in range(n_q - N_H, n_q):
            send_h(q).wait_send()
        for q in range(n_q - N_T, n_q):
            send_t(q).wait_send()
        z_wait(n_q - 2)
        z_wait(n_q - 1)

    blk = (d_blk, fc)
    pl.run_scoped(main, pltpu.VMEM((2, 4) + blk, F32), pltpu.VMEM((4,) + blk, F32), pltpu.VMEM((N_K, 2) + blk, F32),
                  pltpu.VMEM((N_H, 2) + blk, F32), pltpu.VMEM((N_T,) + blk, F32), pltpu.VMEM((2,) + blk, F32),
                  pltpu.VMEM((4,) + blk, F32), pltpu.VMEM((2,) + blk, F32), pltpu.VMEM(blk, F32),
                  pltpu.VMEM((tokens, fc), BF16), pltpu.VMEM((8, r2, tokens), BF16),
                  pltpu.VMEM((fc, d_model), BF16), pltpu.VMEM((tokens, fc), BF16),
                  pltpu.VMEM((fc, d_model), BF16), pltpu.VMEM((tokens, fc), BF16))

    for kind in range(7):
        for p in range(n_piece):
            w1_copy(kind, p, me, sib).wait_send()
            w2_copy(kind, p, me, sib).wait_send()


def fused_step(w1, w2, x, g):
    tokens, d_model = x.shape
    d_ff = w1.shape[1]
    fc = d_ff // N_CHUNK
    d_blk = d_model // 8
    n_q = 2 * N_CHUNK
    shape = jax.ShapeDtypeStruct
    any_spec = pl.BlockSpec(memory_space=pl.ANY)
    dma = pltpu.SemaphoreType.DMA
    out_shape = (
        shape((tokens, d_model), BF16),
        shape((d_blk, d_ff), F32),
        shape((d_ff // 8, d_model), F32),
        shape((8, d_blk, d_ff), BF16),
        shape((d_ff, d_model), BF16),
        shape((tokens, d_ff), BF16),
        shape((tokens, d_ff), BF16),
        shape((d_ff, tokens), BF16),
        shape((n_q, 4, d_blk, fc), F32),
        shape((n_q, 2, d_blk, fc), F32),
        shape((n_q, d_blk, fc), F32),
    )
    outs = pl.pallas_call(
        functools.partial(kernel, (tokens, d_model, d_ff)),
        out_shape=out_shape,
        in_specs=[any_spec] * 4,
        out_specs=tuple([any_spec] * len(out_shape)),
        scratch_shapes=[
            pltpu.VMEM((tokens, d_model), BF16),
            pltpu.VMEM((tokens, d_model), BF16),
            pltpu.VMEM((tokens, d_model), F32),
            dma((7, 4)), dma((7, 4)), dma((7, 4)), dma((7, 4)),
            dma((3, n_q)), dma((2,)), dma((N_H,)), dma((N_T,)),
            dma((3, 2)), dma((2,)), dma((4,)), dma((5,)),
        ],
        compiler_params=pltpu.CompilerParams(collective_id=0, has_side_effects=True, vmem_limit_bytes=67000000),
        name="mlp_step",
    )(w1, w2, x, g)
    return outs[0], outs[1], outs[2]


def solution(mesh):
    row_spec = P(None, 'fsdp', None)

    def per_device(w_up, w_down, tokens_in, cotangent):
        width = tokens_in.shape[-1]
        y, gup, gdown = fused_step(w_up[0], w_down[0], tokens_in.reshape(-1, width), cotangent.reshape(-1, width))
        return y.reshape(tokens_in.shape), gup[None], gdown[None]

    return jax.shard_map(per_device, mesh=mesh, in_specs=(row_spec,) * 4, out_specs=(row_spec,) * 3, check_vma=False)
```

```python
import functools
import math

import jax
import jax.numpy as jnp
from jax import lax
from jax.experimental import pallas as pl
from jax.experimental.pallas import tpu as pltpu
from jax.sharding import PartitionSpec as P

F32 = jnp.float32
BF16 = jnp.bfloat16
N_CHUNK = 11
LAG_H = 2
LAG_T = 4
LAG_Z = 8
N_K = 8
N_H = 3
N_T = 4
Y_STEP = 6
GELU_C = math.sqrt(2.0 / math.pi)
NN = (((1,), (0,)), ((), ()))
NT_DIMS = (((1,), (1,)), ((), ()))
TN_DIMS = (((0,), (0,)), ((), ()))


def matmul(a, b, dims=NN):
    return lax.dot_general(a, b, dims, preferred_element_type=F32)


def aligned(start, size):
    return pl.ds(pl.multiple_of(start, size), size)


def kernel(sizes, w1, w2, x, g, y, gup, gdown, w1f, w2f, a_h, h_h, ht_h, r_s, r_h, r_t,
           x_v, g_v, y_acc, w1_ss, w1_rs, w2_ss, w2_rs, c_rs, s_ss, h_ss, t_ss, loc, out_sem, io_sem, ld_sem):
    tokens, d_model, d_ff = sizes
    fc = d_ff // N_CHUNK
    d_blk = d_model // 8
    f_blk = d_ff // 8
    r2 = f_blk // N_CHUNK
    n_tile = d_model // fc
    n_q = 2 * N_CHUNK
    row_t = tokens // 3
    n_row = 3
    pieces = ((0, 2), (2, 3), (5, 3), (8, 3))
    n_piece = 4
    p_rows = f_blk // n_piece

    me = lax.axis_index('fsdp')
    core = me % 2
    cx = (me // 2) % 2
    cy = me // 4
    chip = me // 2

    def dev(flip_y, flip_x, flip_c):
        yy = 1 - cy if flip_y else cy
        xx = 1 - cx if flip_x else cx
        cc = 1 - core if flip_c else core
        return 4 * yy + 2 * xx + cc

    sib, xn, yn = dev(0, 0, 1), dev(0, 1, 0), dev(1, 0, 0)
    diag = dev(1, 1, 0)
    origins = (xn, yn, diag, sib, dev(0, 1, 1), dev(1, 0, 1), dev(1, 1, 1), diag)

    def remote(src, dst, ssem, rsem, to):
        return pltpu.make_async_remote_copy(src_ref=src, dst_ref=dst, send_sem=ssem, recv_sem=rsem,
                                            device_id=(to,), device_id_type=pl.DeviceIdType.MESH)

    barrier = pltpu.get_barrier_semaphore()
    for other in (sib, xn, yn):
        pl.semaphore_signal(barrier, inc=1, device_id=(other,), device_id_type=pl.DeviceIdType.MESH)
    pl.semaphore_wait(barrier, 3)

    def w1_cols(p):
        return pl.ds(pieces[p][0] * fc, pieces[p][1] * fc)

    half = d_blk // 2

    def w1_copy(kind, p, origin, to, own=False):
        rows = pl.ds(0, half) if kind == 2 else pl.ds(half, half) if kind == 7 else pl.ds(0, d_blk)
        src = w1.at[rows, w1_cols(p)] if own else w1f.at[origin, rows, w1_cols(p)]
        return remote(src, w1f.at[origin, rows, w1_cols(p)], w1_ss.at[kind, p], w1_rs.at[kind, p], to)

    def w2_copy(kind, p, origin, to, own=False):
        rows = aligned(p * p_rows, p_rows)
        full = aligned(origin * f_blk + p * p_rows, p_rows)
        src = w2.at[rows, :] if own else w2f.at[full, :]
        return remote(src, w2f.at[full, :], w2_ss.at[kind, p], w2_rs.at[kind, p], to)

    def w1_recv(kind, p):
        w1_copy(kind, p, origins[kind], me).wait_recv()

    def w2_recv(kind, p):
        w2_copy(kind, p, origins[kind], me).wait_recv()

    def w2_forward(p):
        w2_recv(0, p)
        if p % 2:
            w2_copy(2, p, xn, yn).start()
        w2_copy(4, p, xn, sib).start()
        w2_recv(1, p)
        if not p % 2:
            w2_copy(2, p, yn, xn).start()
        w2_copy(5, p, yn, sib).start()

    def own_w1(p):
        w1_copy(0, p, me, xn, own=True).start()
        w1_copy(1, p, me, yn, own=True).start()

    def own_w2(p):
        w2_copy(0, p, me, xn, own=True).start()
        w2_copy(1, p, me, yn, own=True).start()

    own_w1(0)
    own_w1(1)
    for p in range(n_piece):
        w1_copy(3, p, me, sib, own=True).start()
    for p in range(n_piece):
        w2_copy(3, p, me, sib, own=True).start()

    load_x = pltpu.make_async_copy(x, x_v, io_sem.at[0])
    load_g = pltpu.make_async_copy(g, g_v, io_sem.at[1])
    load_x.start()
    load_g.start()

    def stage_own(buf1, buf2):
        in1 = pltpu.make_async_copy(w1, buf1, io_sem.at[2])
        in2 = pltpu.make_async_copy(w2, buf2, io_sem.at[3])
        in1.start()
        in2.start()
        in1.wait()
        out1 = pltpu.make_async_copy(buf1, w1f.at[me], io_sem.at[2])
        out1.start()
        in2.wait()
        out2 = pltpu.make_async_copy(buf2, w2f.at[aligned(me * f_blk, f_blk), :], io_sem.at[3])
        out2.start()
        out1.wait()
        out2.wait()

    pl.run_scoped(stage_own, pltpu.VMEM((d_blk, d_ff), BF16), pltpu.VMEM((f_blk, d_model), BF16))
    load_x.wait()
    load_g.wait()

    def init_rows(r, _):
        rows = aligned(r * row_t, row_t)
        y_acc[rows, :] = x_v[rows, :].astype(F32)
        return 0

    lax.fori_loop(0, n_row, init_rows, 0)

    def pass_one(wb, ab, hb, htb):
        def w1_load(k, slot):
            return pltpu.make_async_copy(w1f.at[:, :, aligned(k * fc, fc)], wb.at[slot], ld_sem.at[slot])

        def stores(k, slot):
            cols = aligned(k * fc, fc)
            return (pltpu.make_async_copy(ab.at[slot], a_h.at[:, cols], loc.at[0, slot]),
                    pltpu.make_async_copy(hb.at[slot], h_h.at[:, cols], loc.at[1, slot]),
                    pltpu.make_async_copy(htb.at[slot], ht_h.at[cols, :], loc.at[2, slot]))

        def compute(p):
            for kind in (3, 4, 5, 6):
                w1_recv(kind, p)
            first, count = pieces[p]
            w1_load(first, first % 2).start()

            def chunk(k, _):
                slot = k % 2
                w1_load(k, slot).wait()

                @pl.when(k + 1 < first + count)
                def _():
                    w1_load(k + 1, 1 - slot).start()

                @pl.when(k >= 2)
                def _():
                    for cp in stores(k - 2, slot):
                        cp.wait()

                def rows_loop(r, _):
                    rows = aligned(r * row_t, row_t)
                    acc = matmul(x_v[rows, :], wb[slot].reshape(d_model, fc)).astype(BF16)
                    ab[slot, rows, :] = acc
                    u = acc.astype(F32)
                    t = jnp.tanh(GELU_C * (u + 0.044715 * (u * u * u)))
                    hid = (u * (0.5 * (1.0 + t))).astype(BF16)
                    hb[slot, rows, :] = hid
                    htb[slot, :, rows] = hid.T
                    return 0

                lax.fori_loop(0, n_row, rows_loop, 0)
                for cp in stores(k, slot):
                    cp.start()
                return 0

            lax.fori_loop(first, first + count, chunk, 0)

        def diag_forward(p):
            w1_recv(2, p)
            w1_recv(7, p)
            w1_copy(6, p, diag, sib).start()

        for p in range(n_piece):
            w1_recv(0, p)
            w1_copy(7, p, xn, yn).start()
            w1_copy(4, p, xn, sib).start()
            w1_recv(1, p)
            w1_copy(2, p, yn, xn).start()
            w1_copy(5, p, yn, sib).start()
            if p + 2 < n_piece:
                own_w1(p + 2)
            else:
                own_w2(p + 2 - n_piece)
            if p >= 1:
                diag_forward(p - 1)
            if p >= 2:
                compute(p - 2)
        own_w2(2)
        own_w2(3)
        w2_forward(0)
        diag_forward(n_piece - 1)
        compute(n_piece - 2)
        w2_forward(1)
        compute(n_piece - 1)
        w2_forward(2)
        for k in (N_CHUNK - 2, N_CHUNK - 1):
            for cp in stores(k, k % 2):
                cp.wait()

    pl.run_scoped(pass_one, pltpu.VMEM((2, 8, d_blk, fc), BF16), pltpu.VMEM((2, tokens, fc), BF16),
                  pltpu.VMEM((2, tokens, fc), BF16), pltpu.VMEM((2, fc, tokens), BF16))

    def pick(par, even, odd):
        return even * (1 - par) + odd * par

    def first_dev(q):
        return pick(q % 2, xn, yn)

    def second_dev(q):
        return pick(q % 2, yn, xn)

    def chips_of(q):
        return (first_dev(q) // 2, 3 - chip, chip, second_dev(q) // 2)

    def main(s_b, m_b, k_b, h_b, t_b, z_b, st_s, st_h, st_t, q_v, lhs, w2e, a_v, w2y, hy):

        def send_s(q):
            return remote(s_b.at[q % 2], r_s.at[q], s_ss.at[q % 2], c_rs.at[0, q], sib)

        def send_h(q):
            return remote(h_b.at[q % N_H], r_h.at[q], h_ss.at[q % N_H], c_rs.at[1, q], first_dev(q))

        def send_t(q):
            return remote(t_b.at[q % N_T], r_t.at[q], t_ss.at[q % N_T], c_rs.at[2, q], second_dev(q))

        def sib_load(q):
            return pltpu.make_async_copy(r_s.at[q], st_s, io_sem.at[0])

        def lhs_loads(q):
            cps = []
            for b, mb in enumerate(chips_of(q)):
                for j, cc in enumerate((1 - core, core)):
                    rows = aligned(f_blk * (2 * mb + cc) + r2 * q, r2)
                    cps.append(pltpu.make_async_copy(ht_h.at[rows, :], lhs.at[4 * j + b], ld_sem.at[0]))
            return cps

        def lhs_wait():
            pltpu.make_async_copy(lhs, lhs, ld_sem.at[0]).wait()

        def e_loads(k):
            return (pltpu.make_async_copy(w2f.at[aligned(k * fc, fc), :], w2e, ld_sem.at[1]),
                    pltpu.make_async_copy(a_h.at[:, aligned(k * fc, fc)], a_v, ld_sem.at[2]))

        def y_loads(k):
            return (pltpu.make_async_copy(w2f.at[aligned(k * fc, fc), :], w2y, ld_sem.at[3]),
                    pltpu.make_async_copy(h_h.at[:, aligned(k * fc, fc)], hy, ld_sem.at[4]))

        def z_out(q, cond_down):
            slot = q % 2
            if cond_down:
                return [pltpu.make_async_copy(z_b.at[slot, n * r2:(n + 1) * r2, :],
                                              gdown.at[aligned(q * r2, r2), n * fc:(n + 1) * fc], out_sem.at[slot])
                        for n in range(n_tile)]
            return [pltpu.make_async_copy(z_b.at[slot], gup.at[:, aligned((q - N_CHUNK) * fc, fc)], out_sem.at[slot])]

        def z_wait(q):
            pltpu.make_async_copy(z_b.at[q % 2], gup.at[:, pl.ds(0, fc)], out_sem.at[q % 2]).wait()

        for cp in lhs_loads(0):
            cp.start()

        def step(s, _):
            @pl.when(s == 1)
            def _():
                w2_forward(3)

            @pl.when(s == Y_STEP - 1)
            def _():
                for p in range(n_piece):
                    w2_recv(2, p)
                    w2_copy(6, p, diag, sib).start()

            @pl.when(s == Y_STEP)
            def _():
                for p in range(n_piece):
                    for kind in (3, 4, 5, 6):
                        w2_recv(kind, p)
                for cp in y_loads(0):
                    cp.start()
                for cp in e_loads(0):
                    cp.start()

            @pl.when((s >= LAG_H) & (s - LAG_H < n_q))
            def _():
                q = s - LAG_H

                @pl.when(q >= N_H)
                def _():
                    send_h(q - N_H).wait_send()

                sib_load(q).wait()
                h_b[q % N_H] = m_b[q % 2, 0:2] + st_s[0:2]
                send_h(q).start()
                k_b[q % N_K] = m_b[q % 2, 2:4] + st_s[2:4]

            @pl.when((s >= LAG_T) & (s - LAG_T < n_q))
            def _():
                q = s - LAG_T
                send_h(q).wait_recv()
                ld = pltpu.make_async_copy(r_h.at[q], st_h, io_sem.at[1])
                ld.start()

                @pl.when(q >= N_T)
                def _():
                    send_t(q - N_T).wait_send()

                ld.wait()
                t_b[q % N_T] = k_b[q % N_K, 1] + st_h[1]
                send_t(q).start()
                k_b[q % N_K, 0] = k_b[q % N_K, 0] + st_h[0]

            @pl.when(s >= LAG_Z)
            def _():
                q = s - LAG_Z
                send_t(q).wait_recv()
                ld = pltpu.make_async_copy(r_t.at[q], st_t, io_sem.at[2])
                ld.start()

                @pl.when(q >= 2)
                def _():
                    z_wait(q - 2)

                ld.wait()
                z_b[q % 2] = k_b[q % N_K, 0] + st_t[...]

                @pl.when(q < N_CHUNK)
                def _():
                    for cp in z_out(q, True):
                        cp.start()

                @pl.when(q >= N_CHUNK)
                def _():
                    for cp in z_out(q, False):
                        cp.start()

            @pl.when((s >= 2) & (s < n_q))
            def _():
                send_s(s - 2).wait_send()

            @pl.when(s < N_CHUNK)
            def _():
                lhs_wait()

                def tile(n, _):
                    cols = aligned(n * fc, fc)
                    res = matmul(lhs[...].reshape(8 * r2, tokens), g_v[:, cols])
                    rows = aligned(n * r2, r2)
                    for b in range(4):
                        s_b[s % 2, b, rows, :] = res[b * r2:(b + 1) * r2]
                        m_b[s % 2, b, rows, :] = res[(4 + b) * r2:(5 + b) * r2]
                    return 0

                lax.fori_loop(0, n_tile, tile, 0)
                send_s(s).start()

                @pl.when(s + 1 < N_CHUNK)
                def _():
                    for cp in lhs_loads(s + 1):
                        cp.start()

            @pl.when((s >= N_CHUNK) & (s < n_q))
            def _():
                k = s - N_CHUNK
                for cp in e_loads(k):
                    cp.wait()

                def rows_loop(r, _):
                    rows = aligned(r * row_t, row_t)
                    e = matmul(g_v[rows, :], w2e[...], NT_DIMS)
                    u = a_v[rows, :].astype(F32)
                    u2 = u * u
                    t = jnp.tanh(GELU_C * (u + 0.044715 * (u2 * u)))
                    slope = 0.5 * (1.0 + t) + (0.5 * u * (1.0 - t * t)) * GELU_C * (1.0 + 0.134145 * u2)
                    q_v[rows, :] = (e * slope).astype(BF16)
                    return 0

                lax.fori_loop(0, n_row, rows_loop, 0)

                @pl.when(k + 1 < N_CHUNK)
                def _():
                    for cp in e_loads(k + 1):
                        cp.start()

                for b, mb in enumerate(chips_of(s)):
                    for cc, dst in ((1 - core, s_b.at[s % 2]), (core, m_b.at[s % 2])):
                        rows = aligned(d_blk * (2 * mb + cc), d_blk)
                        dst[b] = matmul(x_v[:, rows], q_v[...], TN_DIMS)
                send_s(s).start()

            @pl.when((s >= Y_STEP) & (s < Y_STEP + N_CHUNK))
            def _():
                k = s - Y_STEP
                for cp in y_loads(k):
                    cp.wait()

                def rows_loop(r, _):
                    rows = aligned(r * row_t, row_t)
                    y_acc[rows, :] += matmul(hy[rows, :], w2y[...])
                    return 0

                lax.fori_loop(0, n_row, rows_loop, 0)

                @pl.when(k + 1 < N_CHUNK)
                def _():
                    for cp in y_loads(k + 1):
                        cp.start()

            @pl.when(s == Y_STEP + N_CHUNK)
            def _():
                for n in range(n_tile):
                    hy[...] = y_acc[:, n * fc:(n + 1) * fc].astype(BF16)
                    cp = pltpu.make_async_copy(hy, y.at[:, n * fc:(n + 1) * fc], ld_sem.at[4])
                    cp.start()
                    cp.wait()

            @pl.when((s + 1 >= LAG_H) & (s + 1 - LAG_H < n_q))
            def _():
                send_s(s + 1 - LAG_H).wait_recv()
                sib_load(s + 1 - LAG_H).start()

            return 0

        lax.fori_loop(0, n_q + LAG_Z, step, 0)
        send_s(n_q - 2).wait_send()
        send_s(n_q - 1).wait_send()
        for q in range(n_q - N_H, n_q):
            send_h(q).wait_send()
        for q in range(n_q - N_T, n_q):
            send_t(q).wait_send()
        z_wait(n_q - 2)
        z_wait(n_q - 1)

    blk = (d_blk, fc)
    pl.run_scoped(main, pltpu.VMEM((2, 4) + blk, F32), pltpu.VMEM((2, 4) + blk, F32), pltpu.VMEM((N_K, 2) + blk, F32),
                  pltpu.VMEM((N_H, 2) + blk, F32), pltpu.VMEM((N_T,) + blk, F32), pltpu.VMEM((2,) + blk, F32),
                  pltpu.VMEM((4,) + blk, F32), pltpu.VMEM((2,) + blk, F32), pltpu.VMEM(blk, F32),
                  pltpu.VMEM((tokens, fc), BF16), pltpu.VMEM((8, r2, tokens), BF16),
                  pltpu.VMEM((fc, d_model), BF16), pltpu.VMEM((tokens, fc), BF16),
                  pltpu.VMEM((fc, d_model), BF16), pltpu.VMEM((tokens, fc), BF16))

    for p in range(n_piece):
        for kind in range(8):
            w1_copy(kind, p, me, sib).wait_send()
        for kind in range(7):
            w2_copy(kind, p, me, sib).wait_send()


def fused_step(w1, w2, x, g):
    tokens, d_model = x.shape
    d_ff = w1.shape[1]
    fc = d_ff // N_CHUNK
    d_blk = d_model // 8
    n_q = 2 * N_CHUNK
    shape = jax.ShapeDtypeStruct
    any_spec = pl.BlockSpec(memory_space=pl.ANY)
    dma = pltpu.SemaphoreType.DMA
    out_shape = (
        shape((tokens, d_model), BF16),
        shape((d_blk, d_ff), F32),
        shape((d_ff // 8, d_model), F32),
        shape((8, d_blk, d_ff), BF16),
        shape((d_ff, d_model), BF16),
        shape((tokens, d_ff), BF16),
        shape((tokens, d_ff), BF16),
        shape((d_ff, tokens), BF16),
        shape((n_q, 4, d_blk, fc), F32),
        shape((n_q, 2, d_blk, fc), F32),
        shape((n_q, d_blk, fc), F32),
    )
    outs = pl.pallas_call(
        functools.partial(kernel, (tokens, d_model, d_ff)),
        out_shape=out_shape,
        in_specs=[any_spec] * 4,
        out_specs=tuple([any_spec] * len(out_shape)),
        scratch_shapes=[
            pltpu.VMEM((tokens, d_model), BF16),
            pltpu.VMEM((tokens, d_model), BF16),
            pltpu.VMEM((tokens, d_model), F32),
            dma((8, 4)), dma((8, 4)), dma((7, 4)), dma((7, 4)),
            dma((3, n_q)), dma((2,)), dma((N_H,)), dma((N_T,)),
            dma((3, 2)), dma((2,)), dma((4,)), dma((5,)),
        ],
        compiler_params=pltpu.CompilerParams(collective_id=0, has_side_effects=True, vmem_limit_bytes=67000000),
        name="mlp_step",
    )(w1, w2, x, g)
    return outs[0], outs[1], outs[2]


def solution(mesh):
    row_spec = P(None, 'fsdp', None)

    def per_device(w_up, w_down, tokens_in, cotangent):
        width = tokens_in.shape[-1]
        y, gup, gdown = fused_step(w_up[0], w_down[0], tokens_in.reshape(-1, width), cotangent.reshape(-1, width))
        return y.reshape(tokens_in.shape), gup[None], gdown[None]

    return jax.shard_map(per_device, mesh=mesh, in_specs=(row_spec,) * 4, out_specs=(row_spec,) * 3, check_vma=False)
```

```python
import functools
import math

import jax
import jax.numpy as jnp
from jax import lax
from jax.experimental import pallas as pl
from jax.experimental.pallas import tpu as pltpu
from jax.sharding import PartitionSpec as P

F32 = jnp.float32
BF16 = jnp.bfloat16
N_CHUNK = 11
N_FOUR = 6
N_DOWN = N_CHUNK - N_FOUR
N_PAIR = N_DOWN + N_CHUNK
N_PRE = 5
LAG_Z = 6
N_K = 5
N_H = 6
N_SPLIT = 8
T_STEP = 11
GELU_C = math.sqrt(2.0 / math.pi)
NN = (((1,), (0,)), ((), ()))
NT = (((1,), (1,)), ((), ()))
TN = (((0,), (0,)), ((), ()))


def matmul(a, b, dims=NN):
    return lax.dot_general(a, b, dims, preferred_element_type=F32)


def aligned(start, size):
    return pl.ds(pl.multiple_of(start, size), size)


def gelu_parts(u):
    p = GELU_C + (GELU_C * 0.044715) * (u * u)
    t = jnp.tanh(u * p)
    return t, p


def gelu_hidden(u):
    t, _ = gelu_parts(u)
    return u * (0.5 * (1.0 + t))


def gelu_slope(u):
    t, p = gelu_parts(u)
    return 0.5 * (1.0 + t), (0.5 * u * (1.0 - t * t)) * (3.0 * p - 2.0 * GELU_C)


def kernel(sizes, w1, w2, x, g, y, gup, gdown,
           w1f, w2f, x_l, g_l, a_h, ht_h, a2_h, ht2_h, q_h, q2_h, r_s4, r_h4, r_t4, h_h4, k_h4, t_h4, r_sp, r_hp,
           x_v, g_v, x_n, g_n, y_acc,
           w1_ss, w1_rs, w2_ss, w2_rs, tk_ss, tk_rs, four_ss, four_rs, s_ss, hp_ss, sp_rs, hp_rs, io, ld, out_sem):
    tokens, d_model, d_ff = sizes
    fc = d_ff // N_CHUNK
    hc = fc // 2
    d_blk = d_model // 8
    f_blk = d_ff // 8
    r2 = f_blk // N_CHUNK
    n_tile = d_model // fc
    row_t = tokens // 3
    n_row = 3
    pieces = ((0, 2), (2, 3), (5, 3), (8, 3))
    n_piece = 4
    p_rows = f_blk // n_piece

    me = lax.axis_index('fsdp')
    core = me % 2
    cx = (me // 2) % 2
    cy = me // 4
    chip = me // 2

    def at(yy, xx, cc):
        return 4 * yy + 2 * xx + cc

    oy, ox, oc = 1 - cy, 1 - cx, 1 - core
    sib, xn, yn, diag = at(cy, cx, oc), at(cy, ox, core), at(oy, cx, core), at(oy, ox, core)
    chip_x = xn // 2
    w1_org = (xn, yn, diag, sib, at(cy, ox, oc), at(oy, cx, oc), at(oy, ox, oc))
    w2_org = (xn, at(oy, 0, core), at(oy, 1, core), sib, at(cy, ox, oc), at(oy, 0, oc), at(oy, 1, oc))

    def remote(src, dst, ssem, rsem, to):
        return pltpu.make_async_remote_copy(src_ref=src, dst_ref=dst, send_sem=ssem, recv_sem=rsem,
                                            device_id=(to,), device_id_type=pl.DeviceIdType.MESH)

    def local(src, dst, sem):
        return pltpu.make_async_copy(src, dst, sem)

    barrier = pltpu.get_barrier_semaphore()
    for other in (sib, xn, yn):
        pl.semaphore_signal(barrier, inc=1, device_id=(other,), device_id_type=pl.DeviceIdType.MESH)
    pl.semaphore_wait(barrier, 3)

    def w1_cols(p):
        return pl.ds(pieces[p][0] * fc, pieces[p][1] * fc)

    def w1_copy(kind, p, origin, to, own=False):
        src = w1.at[:, w1_cols(p)] if own else w1f.at[origin, :, w1_cols(p)]
        return remote(src, w1f.at[origin, :, w1_cols(p)], w1_ss.at[kind, p], w1_rs.at[kind, p], to)

    def w2_copy(kind, p, origin, to, own=False):
        rows = aligned(p * p_rows, p_rows)
        full = aligned(origin * f_blk + p * p_rows, p_rows)
        src = w2.at[rows, :] if own else w2f.at[full, :]
        return remote(src, w2f.at[full, :], w2_ss.at[kind, p], w2_rs.at[kind, p], to)

    def token_copy(n):
        src, dst = (x, x_l) if n < 3 else (g, g_l)
        rows = pl.ds((n % 3) * row_t, row_t)
        return remote(src.at[rows, :], dst.at[rows, :], tk_ss.at[n], tk_rs.at[n], yn)

    def w1_recv(kind, p):
        w1_copy(kind, p, w1_org[kind], me).wait_recv()

    def w2_recv(kind, p):
        w2_copy(kind, p, w2_org[kind], me).wait_recv()

    for p in range(n_piece):
        w1_copy(0, p, me, xn, own=True).start()
        w1_copy(1, p, me, yn, own=True).start()
    for n in range(6):
        token_copy(n).start()
    for p in range(n_piece):
        w1_copy(3, p, me, sib, own=True).start()
    for p in range(n_piece):
        w2_copy(3, p, me, sib, own=True).start()

    load_x = local(x, x_v, io.at[0])
    load_g = local(g, g_v, io.at[1])
    load_x.start()
    load_g.start()

    def stage_own(buf1, buf2):
        in1 = local(w1, buf1, io.at[2])
        in2 = local(w2, buf2, io.at[3])
        in1.start()
        in2.start()
        in1.wait()
        out1 = local(buf1, w1f.at[me], io.at[2])
        out1.start()
        in2.wait()
        out2 = local(buf2, w2f.at[aligned(me * f_blk, f_blk), :], io.at[3])
        out2.start()
        out1.wait()
        out2.wait()

    pl.run_scoped(stage_own, pltpu.VMEM((d_blk, d_ff), BF16), pltpu.VMEM((f_blk, d_model), BF16))
    load_x.wait()
    load_g.wait()

    def init_rows(r, c):
        rows = aligned(r * row_t, row_t)
        y_acc[rows, :] = x_v[rows, :].astype(F32)
        return c

    lax.fori_loop(0, n_row, init_rows, ())

    def pass_one(x_ref, a_dst, ht_dst, wb, ab, htb):
        def w1_load(k, slot):
            return local(w1f.at[:, :, aligned(k * fc, fc)], wb.at[slot], ld.at[slot])

        def stores(k, slot):
            cols = aligned(k * fc, fc)
            return (local(ab.at[slot], a_dst.at[:, cols], out_sem.at[slot]),
                    local(htb.at[slot], ht_dst.at[cols, :], out_sem.at[2 + slot]))

        def run(ready):
            def chunk(k, c):
                slot = k % 2
                for p, (first, count) in enumerate(pieces):
                    @pl.when(k == first)
                    def _():
                        ready(p)
                        w1_load(k, slot).start()

                w1_load(k, slot).wait()
                for first, count in pieces:
                    @pl.when((k >= first) & (k + 1 < first + count))
                    def _():
                        w1_load(k + 1, 1 - slot).start()

                @pl.when(k >= 2)
                def _():
                    for cp in stores(k - 2, slot):
                        cp.wait()

                def rows_loop(r, c):
                    rows = aligned(r * row_t, row_t)
                    acc = matmul(x_ref[rows, :], wb[slot].reshape(d_model, fc)).astype(BF16)
                    ab[slot, rows, :] = acc
                    u = acc.astype(F32)
                    htb[slot, :, rows] = gelu_hidden(u).astype(BF16).T
                    return c

                lax.fori_loop(0, n_row, rows_loop, (), unroll=True)
                for cp in stores(k, slot):
                    cp.start()
                return c

            lax.fori_loop(0, N_CHUNK, chunk, ())

        def finish():
            for k in (N_CHUNK - 2, N_CHUNK - 1):
                for cp in stores(k, k % 2):
                    cp.wait()

        return run, finish

    pass_bufs = (pltpu.VMEM((2, 8, d_blk, fc), BF16), pltpu.VMEM((2, tokens, fc), BF16), pltpu.VMEM((2, fc, tokens), BF16))

    def own_pass(wb, ab, htb):
        run, finish = pass_one(x_v, a_h, ht_h, wb, ab, htb)
        for p in range(n_piece):
            w1_recv(0, p)
            w1_copy(4, p, xn, sib).start()
            w1_recv(1, p)
            w1_copy(2, p, yn, xn).start()
            w1_copy(5, p, yn, sib).start()
        for p in range(n_piece):
            w2_copy(0, p, me, xn, own=True).start()
        def ready(p):
            w1_recv(2, p)
            w1_copy(6, p, diag, sib).start()
            for kind in (3, 4, 5, 6):
                w1_recv(kind, p)

        run(ready)
        finish()

    pl.run_scoped(own_pass, *pass_bufs)

    blk = (d_blk, fc)

    def s4_copy(src, q):
        return remote(src, r_s4.at[q], s_ss.at[q % 2], four_rs.at[0, q], sib)

    def h4_copy(q):
        return remote(h_h4.at[q], r_h4.at[q], four_ss.at[0, q], four_rs.at[1, q], xn)

    def t4_copy(q):
        return remote(t_h4.at[q], r_t4.at[q], four_ss.at[1, q], four_rs.at[2, q], yn)

    def lhs_loads(k, chips, src, dst, sem):
        cps = []
        n = len(chips)
        for cc in range(2):
            for b, mb in enumerate(chips):
                rows = aligned(f_blk * (2 * mb + cc) + r2 * k, r2)
                cps.append(local(src.at[rows, :], dst.at[n * cc + b], sem))
        return cps

    def four(sm, st_s, hk, lhs):
        chips = (chip_x, diag // 2, chip, yn // 2)

        def send_s(q):
            return s4_copy(sm.at[q % 2, oc], q)

        def sib_load(q):
            return local(r_s4.at[q], st_s, io.at[0])

        def stores(q):
            return (local(hk.at[q % 2, pl.ds(0, 2)], h_h4.at[q], out_sem.at[q % 2]),
                    local(hk.at[q % 2, pl.ds(2, 2)], k_h4.at[q], out_sem.at[2 + q % 2]))

        for cp in lhs_loads(0, chips, ht_h, lhs, ld.at[0]):
            cp.start()

        def step(s, c):
            @pl.when((s >= 3) & (s - 3 < N_FOUR))
            def _():
                for cp in stores(s - 3):
                    cp.wait()
                h4_copy(s - 3).start()

            @pl.when((s >= 2) & (s - 2 < N_FOUR))
            def _():
                q = s - 2
                sib_load(q).wait()
                hk[q % 2] = sm[q % 2, core] + st_s[...]
                for cp in stores(q):
                    cp.start()
                send_s(q).wait_send()

            @pl.when(s < N_FOUR)
            def _():
                local(lhs, lhs, ld.at[0]).wait()

                def tile(n, c):
                    res = matmul(lhs[...].reshape(8 * r2, tokens), g_v[:, aligned(n * fc, fc)])
                    rows = aligned(n * r2, r2)
                    for b in range(8):
                        sm[s % 2, b // 4, b % 4, rows, :] = res[b * r2:(b + 1) * r2]
                    return c

                lax.fori_loop(0, n_tile, tile, ())
                send_s(s).start()

                @pl.when(s + 1 < N_FOUR)
                def _():
                    for cp in lhs_loads(s + 1, chips, ht_h, lhs, ld.at[0]):
                        cp.start()

            @pl.when((s >= 1) & (s - 1 < N_FOUR))
            def _():
                send_s(s - 1).wait_recv()
                sib_load(s - 1).start()

            return c

        lax.fori_loop(0, N_FOUR + 3, step, ())

    pl.run_scoped(four, pltpu.VMEM((2, 2, 4) + blk, F32), pltpu.VMEM((4,) + blk, F32),
                  pltpu.VMEM((2, 4) + blk, F32), pltpu.VMEM((8, r2, tokens), BF16))

    for p in range(n_piece):
        w2_recv(0, p)
        w2_copy(4, p, xn, sib).start()
    for kind in (1, 2):
        for p in range(n_piece):
            w2_copy(kind, p, at(cy, kind - 1, core), yn).start()

    def half_cols(j, h):
        return aligned((cy * (d_ff // 2) + fc * j + hc * h) % d_ff, hc)

    def y_job(w2c, a_ref):
        def rows_loop(r, c):
            rows = aligned(r * row_t, row_t)
            u = a_ref[rows, :].astype(F32)
            y_acc[rows, :] += matmul(gelu_hidden(u).astype(BF16), w2c[...])
            return c

        lax.fori_loop(0, n_row, rows_loop, (), unroll=True)

    def own_job(w2c, a_ref, q_dst, with_y=True, unroll=False):
        def rows_loop(r, c):
            rows = aligned(r * row_t, row_t)
            e = matmul(g_v[rows, :], w2c[...], NT)
            u = a_ref[rows, :].astype(F32)
            cdf, rest = gelu_slope(u)
            q_dst[rows, :] = (e * (cdf + rest)).astype(BF16)
            if with_y:
                y_acc[rows, :] += matmul((u * cdf).astype(BF16), w2c[...])
            return c

        lax.fori_loop(0, n_row, rows_loop, (), unroll=unroll)

    def nbr_job(w2c, a_ref, q_dst, first, last, unroll=False):
        def rows_loop(r, c):
            rows = aligned(r * row_t, row_t)
            e = matmul(g_n[rows, :], w2c[...], NT)
            cdf, rest = gelu_slope(a_ref[rows, :].astype(F32))
            q_dst[rows, :] = (e * (cdf + rest)).astype(BF16)
            return c

        lax.fori_loop(first, last, rows_loop, (), unroll=unroll)

    def w2_loads(j, dst, sem):
        return [local(w2f.at[half_cols(j, h), :], dst.at[pl.ds(h * hc, hc), :], sem) for h in range(2)]

    def a_loads(j, src, dst, sem):
        return [local(src.at[:, half_cols(j, h)], dst.at[:, pl.ds(h * hc, hc)], sem) for h in range(2)]

    def start_all(cps):
        for cp in cps:
            cp.start()

    def pre_jobs(w2c, a_c, q_c):
        for p in range(n_piece):
            for kind in (3, 4):
                w2_recv(kind, p)
        start_all(w2_loads(0, w2c.at[0], ld.at[0]) + a_loads(0, a_h, a_c.at[0], ld.at[2]))

        def job(j, c):
            slot = j % 2
            local(w2c.at[slot], w2c.at[slot], ld.at[slot]).wait()
            local(a_c.at[slot], a_c.at[slot], ld.at[2 + slot]).wait()

            @pl.when(j + 1 < N_PRE)
            def _():
                start_all(w2_loads(j + 1, w2c.at[1 - slot], ld.at[1 - slot]) +
                          a_loads(j + 1, a_h, a_c.at[1 - slot], ld.at[3 - slot]))

            @pl.when(j >= 2)
            def _():
                local(q_c.at[slot], q_h.at[j - 2], out_sem.at[slot]).wait()

            own_job(w2c.at[slot], a_c.at[slot], q_c.at[slot])
            local(q_c.at[slot], q_h.at[j], out_sem.at[slot]).start()
            return c

        lax.fori_loop(0, N_PRE, job, ())
        for j in (N_PRE - 2, N_PRE - 1):
            local(q_c.at[j % 2], q_h.at[j], out_sem.at[j % 2]).wait()

    pl.run_scoped(pre_jobs, pltpu.VMEM((2, fc, d_model), BF16), pltpu.VMEM((2, tokens, fc), BF16),
                  pltpu.VMEM((2, tokens, fc), BF16))

    for n in range(3):
        token_copy(n).wait_recv()
    cp = local(x_l, x_n, io.at[0])
    cp.start()
    cp.wait()

    def nbr_pass(wb, ab, htb):
        run, finish = pass_one(x_n, a2_h, ht2_h, wb, ab, htb)
        run(lambda p: None)
        finish()

    pl.run_scoped(nbr_pass, *pass_bufs)

    part = tokens - row_t

    def pre_nbr(w2c, a_c, q_c):
        for n in range(3, 5):
            token_copy(n).wait_recv()
        load = local(g_l.at[pl.ds(0, part), :], g_n.at[pl.ds(0, part), :], io.at[2])
        load.start()
        start_all(w2_loads(0, w2c.at[0], ld.at[0]) + a_loads(0, a2_h, a_c.at[0], ld.at[2]))
        load.wait()

        def store(j):
            return local(q_c.at[j % 2, pl.ds(0, part), :], q2_h.at[j], out_sem.at[j % 2])

        def job(j, c):
            slot = j % 2
            local(w2c.at[slot], w2c.at[slot], ld.at[slot]).wait()
            local(a_c.at[slot], a_c.at[slot], ld.at[2 + slot]).wait()

            @pl.when(j + 1 < N_PRE)
            def _():
                start_all(w2_loads(j + 1, w2c.at[1 - slot], ld.at[1 - slot]) +
                          a_loads(j + 1, a2_h, a_c.at[1 - slot], ld.at[3 - slot]))

            @pl.when(j >= 2)
            def _():
                store(j - 2).wait()

            nbr_job(w2c.at[slot], a_c.at[slot], q_c.at[slot], 0, n_row - 1)
            store(j).start()
            return c

        lax.fori_loop(0, N_PRE, job, ())
        for j in (N_PRE - 2, N_PRE - 1):
            store(j).wait()

    pl.run_scoped(pre_nbr, pltpu.VMEM((2, fc, d_model), BF16), pltpu.VMEM((2, tokens, fc), BF16),
                  pltpu.VMEM((2, tokens, fc), BF16))

    def second_sum(q, st_k, st_r):
        h4_copy(q).wait_recv()
        c1 = local(k_h4.at[q], st_k, io.at[2])
        c2 = local(r_h4.at[q], st_r, io.at[3])
        c1.start()
        c2.start()
        c1.wait()
        c2.wait()
        st_r[...] = st_k[...] + st_r[...]
        c1 = local(st_r.at[1], t_h4.at[q], io.at[2])
        c2 = local(st_r.at[0], k_h4.at[q, 0], io.at[3])
        c1.start()
        c2.start()
        c1.wait()
        c2.wait()

    n_early = N_FOUR - 1

    def four_second(st_k, st_r):
        def item(q, c):
            second_sum(q, st_k, st_r)
            return c

        lax.fori_loop(0, n_early, item, ())

    pl.run_scoped(four_second, pltpu.VMEM((2,) + blk, F32), pltpu.VMEM((2,) + blk, F32))

    def pair(sm, h_b, k_b, st_s, st_h, z_b, qa, q_n, lhs, w2c, a_n, qt):
        chips = (chip_x, chip)

        def send_s(i):
            return remote(sm.at[i % 2, oc], r_sp.at[i], s_ss.at[i % 2], sp_rs.at[i], sib)

        def send_h(i):
            return remote(h_b.at[i % N_H], r_hp.at[i], hp_ss.at[i % N_H], hp_rs.at[i], xn)

        def sib_load(i):
            return local(r_sp.at[i], st_s, io.at[0])

        def hop_load(i):
            return local(r_hp.at[i], st_h, io.at[1])

        def mid(s):
            @pl.when((s >= 1) & (s <= N_PAIR))
            def _():
                send_s(s - 1).wait_recv()
                sib_load(s - 1).start()

            @pl.when((s + 1 >= LAG_Z) & (s + 1 - LAG_Z < N_PAIR))
            def _():
                send_h(s + 1 - LAG_Z).wait_recv()
                hop_load(s + 1 - LAG_Z).start()

        def hop(s):
            @pl.when((s >= 1) & (s <= N_PAIR))
            def _():
                i = s - 1

                @pl.when(i >= N_H)
                def _():
                    send_h(i - N_H).wait_send()

                sib_load(i).wait()
                h_b[i % N_H] = sm[i % 2, core, 0] + st_s[0]
                send_h(i).start()
                k_b[i % N_K] = sm[i % 2, core, 1] + st_s[1]

        def last_loads(q):
            slot = q % 2
            return (local(k_h4.at[q, 0], qt.at[slot, 0], io.at[2 + slot]), local(r_t4.at[q], qt.at[slot, 1], io.at[2 + slot]))

        def last_start(q):
            t4_copy(q).wait_recv()
            start_all(last_loads(q))

        def last(q):
            slot = q % 2
            local(qt.at[slot], qt.at[slot], io.at[2 + slot]).wait()
            z_wait(slot)
            z_b[slot] = qt[slot, 0] + qt[slot, 1]
            z_down(q, slot)

        def pair_lhs(i):
            return (lhs_loads(N_FOUR + i, chips, ht_h, lhs.at[0], ld.at[0]) +
                    lhs_loads(N_FOUR + i, chips, ht2_h, lhs.at[1], ld.at[0]))

        def z_wait(slot):
            local(z_b.at[slot], gup.at[:, pl.ds(0, fc)], out_sem.at[slot]).wait()

        def z_down(k, slot):
            start_all([local(z_b.at[slot, n * r2:(n + 1) * r2, :],
                             gdown.at[aligned(k * r2, r2), n * fc:(n + 1) * fc], out_sem.at[slot])
                       for n in range(n_tile)])

        def z_up(j, slot):
            start_all([local(z_b.at[slot, :, h * hc:(h + 1) * hc], gup.at[:, half_cols(j, h)], out_sem.at[slot])
                       for h in range(2)])

        def up_loads(j):
            return w2_loads(j, w2c, ld.at[1]) + a_loads(j, a2_h, a_n, ld.at[2])

        def q2_load(j):
            return local(q2_h.at[j], q_n.at[pl.ds(0, part), :], ld.at[0])

        start_all(pair_lhs(0) + up_loads(0))
        local(q_h.at[0], qa.at[1], ld.at[3]).start()
        token_copy(5).wait_recv()
        load_n = local(g_l.at[pl.ds(part, row_t), :], g_n.at[pl.ds(part, row_t), :], io.at[2])
        load_n.start()
        load_n.wait()

        def step(s, c):
            @pl.when(s >= LAG_Z)
            def _():
                i = s - LAG_Z
                @pl.when(i >= 2)
                def _():
                    z_wait(i % 2)

                hop_load(i).wait()
                z_b[i % 2] = k_b[i % N_K] + st_h[...]

                @pl.when(i < N_DOWN)
                def _():
                    z_down(N_FOUR + i, i % 2)

                @pl.when(i >= N_DOWN)
                def _():
                    z_up(i - N_DOWN, i % 2)

            @pl.when((s >= 2) & (s < N_PAIR))
            def _():
                send_s(s - 2).wait_send()

            @pl.when(s < N_DOWN)
            def _():
                local(lhs, lhs, ld.at[0]).wait()

                @pl.when(s == 1)
                def _():
                    mid(s)
                    hop(s)

                def tile(n, c):
                    cols = aligned(n * fc, fc)
                    rows = aligned(n * r2, r2)
                    res = (matmul(lhs[0].reshape(4 * r2, tokens), g_v[:, cols]) +
                           matmul(lhs[1].reshape(4 * r2, tokens), g_n[:, cols]))
                    for b in range(4):
                        sm[s % 2, b // 2, b % 2, rows, :] = res[b * r2:(b + 1) * r2]

                    @pl.when((n == 1) & (s > 1))
                    def _():
                        mid(s)

                    @pl.when((n == 2) & (s > 1))
                    def _():
                        hop(s)

                    return c

                lax.fori_loop(0, n_tile, tile, ())
                send_s(s).start()

                @pl.when(s + 1 < N_DOWN)
                def _():
                    start_all(pair_lhs(s + 1))

                @pl.when(s + 1 == N_DOWN)
                def _():
                    q2_load(0).start()

            @pl.when(s == N_DOWN + N_PRE - 2)
            def _():
                second_sum(N_FOUR - 1, qt.at[0], qt.at[1])

            @pl.when((s >= T_STEP) & (s < T_STEP + N_FOUR))
            def _():
                t4_copy(s - T_STEP).start()

            @pl.when((s >= N_DOWN) & (s < N_PAIR))
            def _():
                j = s - N_DOWN
                pre = (N_PRE + N_CHUNK - 1 - j) // N_CHUNK
                q_slot = pre * ((j + 1) % 2) + (1 - pre)
                local(w2c, w2c, ld.at[1]).wait()
                local(a_n, a_n, ld.at[2]).wait()
                local(qa.at[0], qa.at[0], ld.at[3]).wait()

                @pl.when(j < N_PRE)
                def _():
                    q2_load(j).wait()


                @pl.when(j < N_PRE)
                def _():
                    nbr_job(w2c, a_n, q_n, n_row - 1, n_row)

                @pl.when(j >= N_PRE)
                def _():
                    nbr_job(w2c, a_n, q_n, 0, n_row, unroll=True)

                mid(s)

                @pl.when(j == N_PRE - 2)
                def _():
                    for p in range(n_piece):
                        w2_recv(1, p)
                        w2_copy(5, p, w2_org[1], sib).start()

                @pl.when((j >= N_PRE) & (j < N_SPLIT))
                def _():
                    own_job(w2c, qa.at[0], qa.at[1])
                    hop(s)

                @pl.when(j >= N_SPLIT)
                def _():
                    own_job(w2c, qa.at[0], qa.at[1], with_y=False, unroll=True)
                    hop(s)

                @pl.when(j == N_SPLIT - 1)
                def _():
                    for p in range(n_piece):
                        w2_recv(2, p)
                        w2_copy(6, p, w2_org[2], sib).start()

                @pl.when(j + 1 == N_PRE)
                def _():
                    for p in range(n_piece):
                        w2_recv(5, p)

                @pl.when((j + 1 < N_CHUNK) & (j + 1 != N_SPLIT))
                def _():
                    start_all(up_loads(j + 1))

                @pl.when(j + 1 < N_PRE)
                def _():
                    local(q_h.at[j + 1], qa.at[j % 2], ld.at[3]).start()

                @pl.when(j + 1 == N_CHUNK)
                def _():
                    start_all(w2_loads(N_SPLIT, w2c, ld.at[1]) + a_loads(N_SPLIT, a_h, qa.at[0], ld.at[3]))

                @pl.when((j + 1 >= N_PRE) & (j + 1 < N_CHUNK))
                def _():
                    start_all(a_loads(j + 1, a_h, qa.at[0], ld.at[3]))

                for b, mb in enumerate(chips):
                    rows = aligned(2 * d_blk * mb, 2 * d_blk)
                    res = matmul(x_v[:, rows], qa[q_slot], TN) + matmul(x_n[:, rows], q_n[...], TN)
                    sm[s % 2, 0, b] = res[:d_blk]
                    sm[s % 2, 1, b] = res[d_blk:]
                send_s(s).start()

                @pl.when(j + 1 < N_PRE)
                def _():
                    q2_load(j + 1).start()

                @pl.when(j < N_PRE)
                def _():
                    hop(s)

                @pl.when(j + 1 == N_SPLIT)
                def _():
                    for p in range(n_piece):
                        w2_recv(6, p)
                    start_all(up_loads(j + 1))

            @pl.when(s >= N_PAIR)
            def _():
                mid(s)
                hop(s)

            n_late = N_CHUNK - N_SPLIT

            @pl.when((s > N_PAIR) & (s <= N_PAIR + n_late))
            def _():
                j = s - N_PAIR - 1 + N_SPLIT
                local(w2c, w2c, ld.at[1]).wait()
                local(qa.at[0], qa.at[0], ld.at[3]).wait()
                y_job(w2c, qa.at[0])

                @pl.when(j + 1 < N_CHUNK)
                def _():
                    start_all(w2_loads(j + 1, w2c, ld.at[1]) + a_loads(j + 1, a_h, qa.at[0], ld.at[3]))

            @pl.when(s == N_PAIR + n_late + 1)
            def _():
                for n in range(n_tile):
                    slot = n % 2
                    if n >= 2:
                        local(qa.at[slot], y.at[:, (n - 2) * fc:(n - 1) * fc], ld.at[2 + slot]).wait()
                    qa[slot] = y_acc[:, n * fc:(n + 1) * fc].astype(BF16)
                    local(qa.at[slot], y.at[:, n * fc:(n + 1) * fc], ld.at[2 + slot]).start()

            for half in range(2):
                @pl.when((s > N_PAIR + 1) & (s < N_PAIR + 2 + N_FOUR // 2))
                def _():
                    last(2 * (s - N_PAIR - 2) + half)

            for half in range(2):
                @pl.when((s > N_PAIR) & (s < N_PAIR + 1 + N_FOUR // 2))
                def _():
                    last_start(2 * (s - N_PAIR - 1) + half)

            return c

        lax.fori_loop(0, N_PAIR + LAG_Z, step, ())
        send_s(N_PAIR - 2).wait_send()
        send_s(N_PAIR - 1).wait_send()
        for i in range(N_PAIR - N_H, N_PAIR):
            send_h(i).wait_send()

        for n in range(n_tile - 2, n_tile):
            local(qa.at[n % 2], y.at[:, n * fc:(n + 1) * fc], ld.at[2 + n % 2]).wait()
        z_wait(0)
        z_wait(1)

    pl.run_scoped(pair, pltpu.VMEM((2, 2, 2) + blk, F32), pltpu.VMEM((N_H,) + blk, F32),
                  pltpu.VMEM((N_K,) + blk, F32), pltpu.VMEM((2,) + blk, F32), pltpu.VMEM(blk, F32),
                  pltpu.VMEM((2,) + blk, F32), pltpu.VMEM((2, tokens, fc), BF16), pltpu.VMEM((tokens, fc), BF16),
                  pltpu.VMEM((2, 4, r2, tokens), BF16), pltpu.VMEM((fc, d_model), BF16),
                  pltpu.VMEM((tokens, fc), BF16), pltpu.VMEM((2, 2) + blk, F32))

    for kind in range(7):
        for p in range(n_piece):
            w1_copy(kind, p, me, sib).wait_send()
            w2_copy(kind, p, me, sib).wait_send()
    for n in range(6):
        token_copy(n).wait_send()
    for q in range(N_FOUR):
        h4_copy(q).wait_send()
        t4_copy(q).wait_send()


def fused_step(w1, w2, x, g):
    tokens, d_model = x.shape
    d_ff = w1.shape[1]
    fc = d_ff // N_CHUNK
    d_blk = d_model // 8
    blk = (d_blk, fc)
    shape = jax.ShapeDtypeStruct
    any_spec = pl.BlockSpec(memory_space=pl.ANY)
    dma = pltpu.SemaphoreType.DMA
    out_shape = (
        shape((tokens, d_model), BF16),
        shape((d_blk, d_ff), F32),
        shape((d_ff // 8, d_model), F32),
        shape((8, d_blk, d_ff), BF16),
        shape((d_ff, d_model), BF16),
        shape((tokens, d_model), BF16),
        shape((tokens, d_model), BF16),
        shape((tokens, d_ff), BF16),
        shape((d_ff, tokens), BF16),
        shape((tokens, d_ff), BF16),
        shape((d_ff, tokens), BF16),
        shape((N_PRE, tokens, fc), BF16),
        shape((N_PRE, tokens - tokens // 3, fc), BF16),
        shape((N_FOUR, 4) + blk, F32),
        shape((N_FOUR, 2) + blk, F32),
        shape((N_FOUR,) + blk, F32),
        shape((N_FOUR, 2) + blk, F32),
        shape((N_FOUR, 2) + blk, F32),
        shape((N_FOUR,) + blk, F32),
        shape((N_PAIR, 2) + blk, F32),
        shape((N_PAIR,) + blk, F32),
    )
    outs = pl.pallas_call(
        functools.partial(kernel, (tokens, d_model, d_ff)),
        out_shape=out_shape,
        in_specs=[any_spec] * 4,
        out_specs=tuple([any_spec] * len(out_shape)),
        scratch_shapes=[
            pltpu.VMEM((tokens, d_model), BF16),
            pltpu.VMEM((tokens, d_model), BF16),
            pltpu.VMEM((tokens, d_model), BF16),
            pltpu.VMEM((tokens, d_model), BF16),
            pltpu.VMEM((tokens, d_model), F32),
            dma((7, 4)), dma((7, 4)), dma((7, 4)), dma((7, 4)), dma((6,)), dma((6,)),
            dma((2, N_FOUR)), dma((3, N_FOUR)), dma((2,)), dma((N_H,)), dma((N_PAIR,)), dma((N_PAIR,)),
            dma((4,)), dma((4,)), dma((4,)),
        ],
        compiler_params=pltpu.CompilerParams(collective_id=0, has_side_effects=True, vmem_limit_bytes=67000000),
        name="mlp_step",
    )(w1, w2, x, g)
    return deliver(outs[0], outs[1], outs[2])


N_PART = 4


def deliver(y, gup, gdown):
    def body(y_in, up_in, down_in, y_out, up_out, down_out, y_buf, up_buf, down_buf, sems_in, sems_out):
        srcs, dsts, bufs = (y_in, up_in, down_in), (y_out, up_out, down_out), (y_buf, up_buf, down_buf)
        moves = []
        for p in range(N_PART):
            for n in range(3):
                rows = srcs[n].shape[0] // N_PART
                part = pl.ds(p * rows, rows)
                moves.append((pltpu.make_async_copy(srcs[n].at[part, :], bufs[n].at[part, :], sems_in.at[n, p]),
                              pltpu.make_async_copy(bufs[n].at[part, :], dsts[n].at[part, :], sems_out.at[n, p])))
        for cp, _ in moves:
            cp.start()
        for cp_in, cp_out in moves:
            cp_in.wait()
            cp_out.start()
        for _, cp in moves:
            cp.wait()

    any_spec = pl.BlockSpec(memory_space=pl.ANY)
    arrays = (y, gup, gdown)
    return pl.pallas_call(
        body,
        out_shape=tuple(jax.ShapeDtypeStruct(a.shape, a.dtype) for a in arrays),
        in_specs=[any_spec] * 3,
        out_specs=(any_spec,) * 3,
        scratch_shapes=[pltpu.VMEM(a.shape, a.dtype) for a in arrays] +
        [pltpu.SemaphoreType.DMA((3, N_PART)), pltpu.SemaphoreType.DMA((3, N_PART))],
        compiler_params=pltpu.CompilerParams(vmem_limit_bytes=60000000),
        name="deliver",
    )(*arrays)


def solution(mesh):
    row_spec = P(None, 'fsdp', None)

    def per_device(w_up, w_down, tokens_in, cotangent):
        width = tokens_in.shape[-1]
        y, gup, gdown = fused_step(w_up[0], w_down[0], tokens_in.reshape(-1, width), cotangent.reshape(-1, width))
        return y.reshape(tokens_in.shape), gup[None], gdown[None]

    return jax.shard_map(per_device, mesh=mesh, in_specs=(row_spec,) * 4, out_specs=(row_spec,) * 3, check_vma=False)
```

```python
import functools
import math

import jax
import jax.numpy as jnp
from jax import lax
from jax.experimental import pallas as pl
from jax.experimental.pallas import tpu as pltpu
from jax.sharding import PartitionSpec as P

F32 = jnp.float32
BF16 = jnp.bfloat16
N_CHUNK = 11
N_FOUR = 6
N_DOWN = N_CHUNK - N_FOUR
N_PAIR = N_DOWN + N_CHUNK
N_PRE = 5
LAG_Z = 6
N_K = 5
N_H = 6
N_SPLIT = 8
T_STEP = 10
GELU_C = math.sqrt(2.0 / math.pi)
NN = (((1,), (0,)), ((), ()))
NT = (((1,), (1,)), ((), ()))
TN = (((0,), (0,)), ((), ()))


def matmul(a, b, dims=NN):
    return lax.dot_general(a, b, dims, preferred_element_type=F32)


def aligned(start, size):
    return pl.ds(pl.multiple_of(start, size), size)


def gelu_parts(u):
    p = GELU_C + (GELU_C * 0.044715) * (u * u)
    t = jnp.tanh(u * p)
    return t, p


def gelu_hidden(u):
    t, _ = gelu_parts(u)
    return u * (0.5 * (1.0 + t))


def gelu_slope(u):
    t, p = gelu_parts(u)
    return 0.5 * (1.0 + t), (0.5 * u * (1.0 - t * t)) * (3.0 * p - 2.0 * GELU_C)


def kernel(sizes, w1, w2, x, g, y, gup, gdown,
           w1f, w2f, x_l, g_l, a_h, ht_h, a2_h, ht2_h, q_h, q2_h, r_s4, r_h4, r_t4, h_h4, k_h4, t_h4, r_sp, r_hp,
           x_v, g_v, x_n, g_n, y_acc,
           w1_ss, w1_rs, w2_ss, w2_rs, tk_ss, tk_rs, four_ss, four_rs, s_ss, hp_ss, sp_rs, hp_rs, io, ld, out_sem):
    tokens, d_model, d_ff = sizes
    fc = d_ff // N_CHUNK
    hc = fc // 2
    d_blk = d_model // 8
    f_blk = d_ff // 8
    r2 = f_blk // N_CHUNK
    n_tile = d_model // fc
    row_t = tokens // 3
    n_row = 3
    pieces = ((0, 2), (2, 3), (5, 3), (8, 3))
    n_piece = 4
    p_rows = f_blk // n_piece

    me = lax.axis_index('fsdp')
    core = me % 2
    cx = (me // 2) % 2
    cy = me // 4
    chip = me // 2

    def at(yy, xx, cc):
        return 4 * yy + 2 * xx + cc

    oy, ox, oc = 1 - cy, 1 - cx, 1 - core
    sib, xn, yn, diag = at(cy, cx, oc), at(cy, ox, core), at(oy, cx, core), at(oy, ox, core)
    chip_x = xn // 2
    w1_org = (xn, yn, diag, sib, at(cy, ox, oc), at(oy, cx, oc), at(oy, ox, oc))
    w2_org = (xn, at(oy, 0, core), at(oy, 1, core), sib, at(cy, ox, oc), at(oy, 0, oc), at(oy, 1, oc))

    def remote(src, dst, ssem, rsem, to):
        return pltpu.make_async_remote_copy(src_ref=src, dst_ref=dst, send_sem=ssem, recv_sem=rsem,
                                            device_id=(to,), device_id_type=pl.DeviceIdType.MESH)

    def local(src, dst, sem):
        return pltpu.make_async_copy(src, dst, sem)

    barrier = pltpu.get_barrier_semaphore()
    for other in (sib, xn, yn):
        pl.semaphore_signal(barrier, inc=1, device_id=(other,), device_id_type=pl.DeviceIdType.MESH)
    pl.semaphore_wait(barrier, 3)

    def w1_cols(p):
        return pl.ds(pieces[p][0] * fc, pieces[p][1] * fc)

    def w1_copy(kind, p, origin, to, own=False):
        src = w1.at[:, w1_cols(p)] if own else w1f.at[origin, :, w1_cols(p)]
        return remote(src, w1f.at[origin, :, w1_cols(p)], w1_ss.at[kind, p], w1_rs.at[kind, p], to)

    def w2_copy(kind, p, origin, to, own=False):
        rows = aligned(p * p_rows, p_rows)
        full = aligned(origin * f_blk + p * p_rows, p_rows)
        src = w2.at[rows, :] if own else w2f.at[full, :]
        return remote(src, w2f.at[full, :], w2_ss.at[kind, p], w2_rs.at[kind, p], to)

    def token_copy(n):
        src, dst = (x, x_l) if n < 3 else (g, g_l)
        rows = pl.ds((n % 3) * row_t, row_t)
        return remote(src.at[rows, :], dst.at[rows, :], tk_ss.at[n], tk_rs.at[n], yn)

    def w1_recv(kind, p):
        w1_copy(kind, p, w1_org[kind], me).wait_recv()

    def w2_recv(kind, p):
        w2_copy(kind, p, w2_org[kind], me).wait_recv()

    for p in range(n_piece):
        w1_copy(0, p, me, xn, own=True).start()
        w1_copy(1, p, me, yn, own=True).start()
    for n in range(6):
        token_copy(n).start()
    for p in range(n_piece):
        w1_copy(3, p, me, sib, own=True).start()
    for p in range(n_piece):
        w2_copy(3, p, me, sib, own=True).start()

    load_x = local(x, x_v, io.at[0])
    load_g = local(g, g_v, io.at[1])
    load_x.start()
    load_g.start()

    def stage_own(buf1, buf2):
        in1 = local(w1, buf1, io.at[2])
        in2 = local(w2, buf2, io.at[3])
        in1.start()
        in2.start()
        in1.wait()
        out1 = local(buf1, w1f.at[me], io.at[2])
        out1.start()
        in2.wait()
        out2 = local(buf2, w2f.at[aligned(me * f_blk, f_blk), :], io.at[3])
        out2.start()
        out1.wait()
        out2.wait()

    pl.run_scoped(stage_own, pltpu.VMEM((d_blk, d_ff), BF16), pltpu.VMEM((f_blk, d_model), BF16))
    load_x.wait()
    load_g.wait()

    def init_rows(r, c):
        rows = aligned(r * row_t, row_t)
        y_acc[rows, :] = x_v[rows, :].astype(F32)
        return c

    lax.fori_loop(0, n_row, init_rows, ())

    def pass_one(x_ref, a_dst, ht_dst, wb, ab, htb):
        def w1_load(k, slot):
            return local(w1f.at[:, :, aligned(k * fc, fc)], wb.at[slot], ld.at[slot])

        def stores(k, slot):
            cols = aligned(k * fc, fc)
            return (local(ab.at[slot], a_dst.at[:, cols], out_sem.at[slot]),
                    local(htb.at[slot], ht_dst.at[cols, :], out_sem.at[2 + slot]))

        def run(ready):
            def chunk(k, c):
                slot = k % 2
                for p, (first, count) in enumerate(pieces):
                    @pl.when(k == first)
                    def _():
                        ready(p)
                        w1_load(k, slot).start()

                w1_load(k, slot).wait()
                for first, count in pieces:
                    @pl.when((k >= first) & (k + 1 < first + count))
                    def _():
                        w1_load(k + 1, 1 - slot).start()

                @pl.when(k >= 2)
                def _():
                    for cp in stores(k - 2, slot):
                        cp.wait()

                def rows_loop(r, c):
                    rows = aligned(r * row_t, row_t)
                    acc = matmul(x_ref[rows, :], wb[slot].reshape(d_model, fc)).astype(BF16)
                    ab[slot, rows, :] = acc
                    u = acc.astype(F32)
                    htb[slot, :, rows] = gelu_hidden(u).astype(BF16).T
                    return c

                lax.fori_loop(0, n_row, rows_loop, (), unroll=True)
                for cp in stores(k, slot):
                    cp.start()
                return c

            lax.fori_loop(0, N_CHUNK, chunk, ())

        def finish():
            for k in (N_CHUNK - 2, N_CHUNK - 1):
                for cp in stores(k, k % 2):
                    cp.wait()

        return run, finish

    pass_bufs = (pltpu.VMEM((2, 8, d_blk, fc), BF16), pltpu.VMEM((2, tokens, fc), BF16), pltpu.VMEM((2, fc, tokens), BF16))

    def own_pass(wb, ab, htb):
        run, finish = pass_one(x_v, a_h, ht_h, wb, ab, htb)
        for p in range(n_piece):
            w1_recv(0, p)
            w1_copy(4, p, xn, sib).start()
            w1_recv(1, p)
            w1_copy(2, p, yn, xn).start()
            w1_copy(5, p, yn, sib).start()
        for p in range(n_piece):
            w2_copy(0, p, me, xn, own=True).start()
        def ready(p):
            w1_recv(2, p)
            w1_copy(6, p, diag, sib).start()
            for kind in (3, 4, 5, 6):
                w1_recv(kind, p)

        run(ready)
        finish()

    pl.run_scoped(own_pass, *pass_bufs)

    blk = (d_blk, fc)

    def s4_copy(src, q):
        return remote(src, r_s4.at[q], s_ss.at[q % 2], four_rs.at[0, q], sib)

    def h4_copy(q):
        return remote(h_h4.at[q], r_h4.at[q], four_ss.at[0, q], four_rs.at[1, q], xn)

    def t4_copy(q):
        return remote(t_h4.at[q], r_t4.at[q], four_ss.at[1, q], four_rs.at[2, q], yn)

    def lhs_loads(k, chips, src, dst, sem):
        cps = []
        n = len(chips)
        for cc in range(2):
            for b, mb in enumerate(chips):
                rows = aligned(f_blk * (2 * mb + cc) + r2 * k, r2)
                cps.append(local(src.at[rows, :], dst.at[n * cc + b], sem))
        return cps

    def four(sm, st_s, hk, lhs):
        chips = (chip_x, diag // 2, chip, yn // 2)

        def send_s(q):
            return s4_copy(sm.at[q % 2, oc], q)

        def sib_load(q):
            return local(r_s4.at[q], st_s, io.at[0])

        def stores(q):
            return (local(hk.at[q % 2, pl.ds(0, 2)], h_h4.at[q], out_sem.at[q % 2]),
                    local(hk.at[q % 2, pl.ds(2, 2)], k_h4.at[q], out_sem.at[2 + q % 2]))

        for cp in lhs_loads(0, chips, ht_h, lhs, ld.at[0]):
            cp.start()

        def step(s, c):
            @pl.when((s >= 3) & (s - 3 < N_FOUR))
            def _():
                for cp in stores(s - 3):
                    cp.wait()
                h4_copy(s - 3).start()

            @pl.when((s >= 2) & (s - 2 < N_FOUR))
            def _():
                q = s - 2
                sib_load(q).wait()
                hk[q % 2] = sm[q % 2, core] + st_s[...]
                for cp in stores(q):
                    cp.start()
                send_s(q).wait_send()

            @pl.when(s < N_FOUR)
            def _():
                local(lhs, lhs, ld.at[0]).wait()

                def tile(n, c):
                    res = matmul(lhs[...].reshape(8 * r2, tokens), g_v[:, aligned(n * fc, fc)])
                    rows = aligned(n * r2, r2)
                    for b in range(8):
                        sm[s % 2, b // 4, b % 4, rows, :] = res[b * r2:(b + 1) * r2]
                    return c

                lax.fori_loop(0, n_tile, tile, ())
                send_s(s).start()

                @pl.when(s + 1 < N_FOUR)
                def _():
                    for cp in lhs_loads(s + 1, chips, ht_h, lhs, ld.at[0]):
                        cp.start()

            @pl.when((s >= 1) & (s - 1 < N_FOUR))
            def _():
                send_s(s - 1).wait_recv()
                sib_load(s - 1).start()

            return c

        lax.fori_loop(0, N_FOUR + 3, step, ())

    pl.run_scoped(four, pltpu.VMEM((2, 2, 4) + blk, F32), pltpu.VMEM((4,) + blk, F32),
                  pltpu.VMEM((2, 4) + blk, F32), pltpu.VMEM((8, r2, tokens), BF16))

    for p in range(n_piece):
        w2_recv(0, p)
        w2_copy(4, p, xn, sib).start()
    for kind in (1, 2):
        for p in range(n_piece):
            w2_copy(kind, p, at(cy, kind - 1, core), yn).start()

    def half_cols(j, h):
        return aligned((cy * (d_ff // 2) + fc * j + hc * h) % d_ff, hc)

    def y_job(w2c, a_ref):
        def rows_loop(r, c):
            rows = aligned(r * row_t, row_t)
            u = a_ref[rows, :].astype(F32)
            y_acc[rows, :] += matmul(gelu_hidden(u).astype(BF16), w2c[...])
            return c

        lax.fori_loop(0, n_row, rows_loop, (), unroll=True)

    def own_job(w2c, a_ref, q_dst, with_y=True, unroll=False):
        def rows_loop(r, c):
            rows = aligned(r * row_t, row_t)
            e = matmul(g_v[rows, :], w2c[...], NT)
            u = a_ref[rows, :].astype(F32)
            cdf, rest = gelu_slope(u)
            q_dst[rows, :] = (e * (cdf + rest)).astype(BF16)
            if with_y:
                y_acc[rows, :] += matmul((u * cdf).astype(BF16), w2c[...])
            return c

        lax.fori_loop(0, n_row, rows_loop, (), unroll=unroll)

    def nbr_job(w2c, a_ref, q_dst, first, last, unroll=False):
        def rows_loop(r, c):
            rows = aligned(r * row_t, row_t)
            e = matmul(g_n[rows, :], w2c[...], NT)
            cdf, rest = gelu_slope(a_ref[rows, :].astype(F32))
            q_dst[rows, :] = (e * (cdf + rest)).astype(BF16)
            return c

        lax.fori_loop(first, last, rows_loop, (), unroll=unroll)

    def w2_loads(j, dst, sem):
        return [local(w2f.at[half_cols(j, h), :], dst.at[pl.ds(h * hc, hc), :], sem) for h in range(2)]

    def a_loads(j, src, dst, sem):
        return [local(src.at[:, half_cols(j, h)], dst.at[:, pl.ds(h * hc, hc)], sem) for h in range(2)]

    def start_all(cps):
        for cp in cps:
            cp.start()

    def pre_jobs(w2c, a_c, q_c):
        for p in range(n_piece):
            for kind in (3, 4):
                w2_recv(kind, p)
        start_all(w2_loads(0, w2c.at[0], ld.at[0]) + a_loads(0, a_h, a_c.at[0], ld.at[2]))

        def job(j, c):
            slot = j % 2
            local(w2c.at[slot], w2c.at[slot], ld.at[slot]).wait()
            local(a_c.at[slot], a_c.at[slot], ld.at[2 + slot]).wait()

            @pl.when(j + 1 < N_PRE)
            def _():
                start_all(w2_loads(j + 1, w2c.at[1 - slot], ld.at[1 - slot]) +
                          a_loads(j + 1, a_h, a_c.at[1 - slot], ld.at[3 - slot]))

            @pl.when(j >= 2)
            def _():
                local(q_c.at[slot], q_h.at[j - 2], out_sem.at[slot]).wait()

            own_job(w2c.at[slot], a_c.at[slot], q_c.at[slot])
            local(q_c.at[slot], q_h.at[j], out_sem.at[slot]).start()
            return c

        lax.fori_loop(0, N_PRE, job, ())
        for j in (N_PRE - 2, N_PRE - 1):
            local(q_c.at[j % 2], q_h.at[j], out_sem.at[j % 2]).wait()

    pl.run_scoped(pre_jobs, pltpu.VMEM((2, fc, d_model), BF16), pltpu.VMEM((2, tokens, fc), BF16),
                  pltpu.VMEM((2, tokens, fc), BF16))

    for n in range(3):
        token_copy(n).wait_recv()
    cp = local(x_l, x_n, io.at[0])
    cp.start()
    cp.wait()

    def nbr_pass(wb, ab, htb):
        run, finish = pass_one(x_n, a2_h, ht2_h, wb, ab, htb)
        run(lambda p: None)
        finish()

    pl.run_scoped(nbr_pass, *pass_bufs)

    part = tokens - row_t

    def pre_nbr(w2c, a_c, q_c):
        for n in range(3, 5):
            token_copy(n).wait_recv()
        load = local(g_l.at[pl.ds(0, part), :], g_n.at[pl.ds(0, part), :], io.at[2])
        load.start()
        start_all(w2_loads(0, w2c.at[0], ld.at[0]) + a_loads(0, a2_h, a_c.at[0], ld.at[2]))
        load.wait()

        def store(j):
            return local(q_c.at[j % 2, pl.ds(0, part), :], q2_h.at[j], out_sem.at[j % 2])

        def job(j, c):
            slot = j % 2
            local(w2c.at[slot], w2c.at[slot], ld.at[slot]).wait()
            local(a_c.at[slot], a_c.at[slot], ld.at[2 + slot]).wait()

            @pl.when(j + 1 < N_PRE)
            def _():
                start_all(w2_loads(j + 1, w2c.at[1 - slot], ld.at[1 - slot]) +
                          a_loads(j + 1, a2_h, a_c.at[1 - slot], ld.at[3 - slot]))

            @pl.when(j >= 2)
            def _():
                store(j - 2).wait()

            nbr_job(w2c.at[slot], a_c.at[slot], q_c.at[slot], 0, n_row - 1)
            store(j).start()
            return c

        lax.fori_loop(0, N_PRE, job, ())
        for j in (N_PRE - 2, N_PRE - 1):
            store(j).wait()

    pl.run_scoped(pre_nbr, pltpu.VMEM((2, fc, d_model), BF16), pltpu.VMEM((2, tokens, fc), BF16),
                  pltpu.VMEM((2, tokens, fc), BF16))

    def second_sum(q, st_k, st_r):
        h4_copy(q).wait_recv()
        c1 = local(k_h4.at[q], st_k, io.at[2])
        c2 = local(r_h4.at[q], st_r, io.at[3])
        c1.start()
        c2.start()
        c1.wait()
        c2.wait()
        st_r[...] = st_k[...] + st_r[...]
        c1 = local(st_r.at[1], t_h4.at[q], io.at[2])
        c2 = local(st_r.at[0], k_h4.at[q, 0], io.at[3])
        c1.start()
        c2.start()
        c1.wait()
        c2.wait()

    n_early = N_FOUR - 1

    def four_second(st_k, st_r):
        def item(q, c):
            second_sum(q, st_k, st_r)
            return c

        lax.fori_loop(0, n_early, item, ())

    pl.run_scoped(four_second, pltpu.VMEM((2,) + blk, F32), pltpu.VMEM((2,) + blk, F32))

    def pair(sm, h_b, k_b, st_s, st_h, z_b, qa, q_n, lhs, w2c, a_n, qt):
        chips = (chip_x, chip)

        def send_s(i):
            return remote(sm.at[i % 2, oc], r_sp.at[i], s_ss.at[i % 2], sp_rs.at[i], sib)

        def send_h(i):
            return remote(h_b.at[i % N_H], r_hp.at[i], hp_ss.at[i % N_H], hp_rs.at[i], xn)

        def sib_load(i):
            return local(r_sp.at[i], st_s, io.at[0])

        def hop_load(i):
            return local(r_hp.at[i], st_h, io.at[1])

        def mid(s):
            @pl.when((s >= 1) & (s <= N_PAIR))
            def _():
                send_s(s - 1).wait_recv()
                sib_load(s - 1).start()

            @pl.when((s + 1 >= LAG_Z) & (s + 1 - LAG_Z < N_PAIR))
            def _():
                send_h(s + 1 - LAG_Z).wait_recv()
                hop_load(s + 1 - LAG_Z).start()

        def hop(s):
            @pl.when((s >= 1) & (s <= N_PAIR))
            def _():
                i = s - 1

                @pl.when(i >= N_H)
                def _():
                    send_h(i - N_H).wait_send()

                sib_load(i).wait()
                h_b[i % N_H] = sm[i % 2, core, 0] + st_s[0]
                send_h(i).start()
                k_b[i % N_K] = sm[i % 2, core, 1] + st_s[1]

        def last_loads(q):
            slot = q % 2
            return (local(k_h4.at[q, 0], qt.at[slot, 0], io.at[2 + slot]), local(r_t4.at[q], qt.at[slot, 1], io.at[2 + slot]))

        def last_start(q):
            t4_copy(q).wait_recv()
            start_all(last_loads(q))

        def last(q):
            slot = q % 2
            local(qt.at[slot], qt.at[slot], io.at[2 + slot]).wait()
            z_wait(slot)
            z_b[slot] = qt[slot, 0] + qt[slot, 1]
            z_down(q, slot)

        def pair_lhs(i):
            return (lhs_loads(N_FOUR + i, chips, ht_h, lhs.at[0], ld.at[0]) +
                    lhs_loads(N_FOUR + i, chips, ht2_h, lhs.at[1], ld.at[0]))

        def z_wait(slot):
            local(z_b.at[slot], gup.at[:, pl.ds(0, fc)], out_sem.at[slot]).wait()

        def z_down(k, slot):
            start_all([local(z_b.at[slot, n * r2:(n + 1) * r2, :],
                             gdown.at[aligned(k * r2, r2), n * fc:(n + 1) * fc], out_sem.at[slot])
                       for n in range(n_tile)])

        def z_up(j, slot):
            start_all([local(z_b.at[slot, :, h * hc:(h + 1) * hc], gup.at[:, half_cols(j, h)], out_sem.at[slot])
                       for h in range(2)])

        def up_loads(j):
            return w2_loads(j, w2c, ld.at[1]) + a_loads(j, a2_h, a_n, ld.at[2])

        def q2_load(j):
            return local(q2_h.at[j], q_n.at[pl.ds(0, part), :], ld.at[0])

        start_all(pair_lhs(0) + up_loads(0))
        local(q_h.at[0], qa.at[1], ld.at[3]).start()
        token_copy(5).wait_recv()
        load_n = local(g_l.at[pl.ds(part, row_t), :], g_n.at[pl.ds(part, row_t), :], io.at[2])
        load_n.start()
        load_n.wait()

        def step(s, c):
            @pl.when(s >= LAG_Z)
            def _():
                i = s - LAG_Z
                @pl.when(i >= 2)
                def _():
                    z_wait(i % 2)

                hop_load(i).wait()
                z_b[i % 2] = k_b[i % N_K] + st_h[...]

                @pl.when(i < N_DOWN)
                def _():
                    z_down(N_FOUR + i, i % 2)

                @pl.when(i >= N_DOWN)
                def _():
                    z_up(i - N_DOWN, i % 2)

            @pl.when((s >= 2) & (s < N_PAIR))
            def _():
                send_s(s - 2).wait_send()

            @pl.when(s < N_DOWN)
            def _():
                local(lhs, lhs, ld.at[0]).wait()

                @pl.when(s == 1)
                def _():
                    mid(s)
                    hop(s)

                def tile(n, c):
                    cols = aligned(n * fc, fc)
                    rows = aligned(n * r2, r2)
                    res = (matmul(lhs[0].reshape(4 * r2, tokens), g_v[:, cols]) +
                           matmul(lhs[1].reshape(4 * r2, tokens), g_n[:, cols]))
                    for b in range(4):
                        sm[s % 2, b // 2, b % 2, rows, :] = res[b * r2:(b + 1) * r2]

                    @pl.when((n == 1) & (s > 1))
                    def _():
                        mid(s)

                    @pl.when((n == 2) & (s > 1))
                    def _():
                        hop(s)

                    return c

                lax.fori_loop(0, n_tile, tile, ())
                send_s(s).start()

                @pl.when(s + 1 < N_DOWN)
                def _():
                    start_all(pair_lhs(s + 1))

                @pl.when(s + 1 == N_DOWN)
                def _():
                    q2_load(0).start()

            @pl.when(s == N_DOWN + N_PRE - 2)
            def _():
                second_sum(N_FOUR - 1, qt.at[0], qt.at[1])

            @pl.when((s >= T_STEP) & (s < T_STEP + N_FOUR))
            def _():
                t4_copy(s - T_STEP).start()

            @pl.when((s >= N_DOWN) & (s < N_PAIR))
            def _():
                j = s - N_DOWN
                pre = (N_PRE + N_CHUNK - 1 - j) // N_CHUNK
                q_slot = pre * ((j + 1) % 2) + (1 - pre)
                local(w2c, w2c, ld.at[1]).wait()
                local(a_n, a_n, ld.at[2]).wait()
                local(qa.at[0], qa.at[0], ld.at[3]).wait()

                @pl.when(j < N_PRE)
                def _():
                    q2_load(j).wait()


                @pl.when(j < N_PRE)
                def _():
                    nbr_job(w2c, a_n, q_n, n_row - 1, n_row)

                @pl.when(j >= N_PRE)
                def _():
                    nbr_job(w2c, a_n, q_n, 0, n_row, unroll=True)

                mid(s)

                @pl.when(j == N_PRE - 2)
                def _():
                    for p in range(n_piece):
                        w2_recv(1, p)
                        w2_copy(5, p, w2_org[1], sib).start()

                @pl.when((j >= N_PRE) & (j < N_SPLIT))
                def _():
                    own_job(w2c, qa.at[0], qa.at[1])
                    hop(s)

                @pl.when(j >= N_SPLIT)
                def _():
                    own_job(w2c, qa.at[0], qa.at[1], with_y=False, unroll=True)
                    hop(s)

                @pl.when(j == N_SPLIT - 1)
                def _():
                    for p in range(n_piece):
                        w2_recv(2, p)
                        w2_copy(6, p, w2_org[2], sib).start()

                @pl.when(j + 1 == N_PRE)
                def _():
                    for p in range(n_piece):
                        w2_recv(5, p)

                @pl.when((j + 1 < N_CHUNK) & (j + 1 != N_SPLIT))
                def _():
                    start_all(up_loads(j + 1))

                @pl.when(j + 1 < N_PRE)
                def _():
                    local(q_h.at[j + 1], qa.at[j % 2], ld.at[3]).start()

                @pl.when(j + 1 == N_CHUNK)
                def _():
                    start_all(w2_loads(N_SPLIT, w2c, ld.at[1]) + a_loads(N_SPLIT, a_h, qa.at[0], ld.at[3]))

                @pl.when((j + 1 >= N_PRE) & (j + 1 < N_CHUNK))
                def _():
                    start_all(a_loads(j + 1, a_h, qa.at[0], ld.at[3]))

                for b, mb in enumerate(chips):
                    rows = aligned(2 * d_blk * mb, 2 * d_blk)
                    res = matmul(x_v[:, rows], qa[q_slot], TN) + matmul(x_n[:, rows], q_n[...], TN)
                    sm[s % 2, 0, b] = res[:d_blk]
                    sm[s % 2, 1, b] = res[d_blk:]
                send_s(s).start()

                @pl.when(j + 1 < N_PRE)
                def _():
                    q2_load(j + 1).start()

                @pl.when(j < N_PRE)
                def _():
                    hop(s)

                @pl.when(j + 1 == N_SPLIT)
                def _():
                    for p in range(n_piece):
                        w2_recv(6, p)
                    start_all(up_loads(j + 1))

            @pl.when(s >= N_PAIR)
            def _():
                mid(s)
                hop(s)

            n_late = N_CHUNK - N_SPLIT

            @pl.when((s > N_PAIR) & (s <= N_PAIR + n_late))
            def _():
                j = s - N_PAIR - 1 + N_SPLIT
                local(w2c, w2c, ld.at[1]).wait()
                local(qa.at[0], qa.at[0], ld.at[3]).wait()
                y_job(w2c, qa.at[0])

                @pl.when(j + 1 < N_CHUNK)
                def _():
                    start_all(w2_loads(j + 1, w2c, ld.at[1]) + a_loads(j + 1, a_h, qa.at[0], ld.at[3]))

            @pl.when(s == N_PAIR + n_late + 1)
            def _():
                for n in range(n_tile):
                    slot = n % 2
                    if n >= 2:
                        local(qa.at[slot], y.at[:, (n - 2) * fc:(n - 1) * fc], ld.at[2 + slot]).wait()
                    qa[slot] = y_acc[:, n * fc:(n + 1) * fc].astype(BF16)
                    local(qa.at[slot], y.at[:, n * fc:(n + 1) * fc], ld.at[2 + slot]).start()

            for half in range(2):
                @pl.when((s > N_PAIR + 1) & (s < N_PAIR + 2 + N_FOUR // 2))
                def _():
                    last(2 * (s - N_PAIR - 2) + half)

            for half in range(2):
                @pl.when((s > N_PAIR) & (s < N_PAIR + 1 + N_FOUR // 2))
                def _():
                    last_start(2 * (s - N_PAIR - 1) + half)

            return c

        lax.fori_loop(0, N_PAIR + LAG_Z, step, ())
        send_s(N_PAIR - 2).wait_send()
        send_s(N_PAIR - 1).wait_send()
        for i in range(N_PAIR - N_H, N_PAIR):
            send_h(i).wait_send()

        for n in range(n_tile - 2, n_tile):
            local(qa.at[n % 2], y.at[:, n * fc:(n + 1) * fc], ld.at[2 + n % 2]).wait()
        z_wait(0)
        z_wait(1)

    pl.run_scoped(pair, pltpu.VMEM((2, 2, 2) + blk, F32), pltpu.VMEM((N_H,) + blk, F32),
                  pltpu.VMEM((N_K,) + blk, F32), pltpu.VMEM((2,) + blk, F32), pltpu.VMEM(blk, F32),
                  pltpu.VMEM((2,) + blk, F32), pltpu.VMEM((2, tokens, fc), BF16), pltpu.VMEM((tokens, fc), BF16),
                  pltpu.VMEM((2, 4, r2, tokens), BF16), pltpu.VMEM((fc, d_model), BF16),
                  pltpu.VMEM((tokens, fc), BF16), pltpu.VMEM((2, 2) + blk, F32))

    for kind in range(7):
        for p in range(n_piece):
            w1_copy(kind, p, me, sib).wait_send()
            w2_copy(kind, p, me, sib).wait_send()
    for n in range(6):
        token_copy(n).wait_send()
    for q in range(N_FOUR):
        h4_copy(q).wait_send()
        t4_copy(q).wait_send()


def fused_step(w1, w2, x, g):
    tokens, d_model = x.shape
    d_ff = w1.shape[1]
    fc = d_ff // N_CHUNK
    d_blk = d_model // 8
    blk = (d_blk, fc)
    shape = jax.ShapeDtypeStruct
    any_spec = pl.BlockSpec(memory_space=pl.ANY)
    dma = pltpu.SemaphoreType.DMA
    out_shape = (
        shape((tokens, d_model), BF16),
        shape((d_blk, d_ff), F32),
        shape((d_ff // 8, d_model), F32),
        shape((8, d_blk, d_ff), BF16),
        shape((d_ff, d_model), BF16),
        shape((tokens, d_model), BF16),
        shape((tokens, d_model), BF16),
        shape((tokens, d_ff), BF16),
        shape((d_ff, tokens), BF16),
        shape((tokens, d_ff), BF16),
        shape((d_ff, tokens), BF16),
        shape((N_PRE, tokens, fc), BF16),
        shape((N_PRE, tokens - tokens // 3, fc), BF16),
        shape((N_FOUR, 4) + blk, F32),
        shape((N_FOUR, 2) + blk, F32),
        shape((N_FOUR,) + blk, F32),
        shape((N_FOUR, 2) + blk, F32),
        shape((N_FOUR, 2) + blk, F32),
        shape((N_FOUR,) + blk, F32),
        shape((N_PAIR, 2) + blk, F32),
        shape((N_PAIR,) + blk, F32),
    )
    outs = pl.pallas_call(
        functools.partial(kernel, (tokens, d_model, d_ff)),
        out_shape=out_shape,
        in_specs=[any_spec] * 4,
        out_specs=tuple([any_spec] * len(out_shape)),
        scratch_shapes=[
            pltpu.VMEM((tokens, d_model), BF16),
            pltpu.VMEM((tokens, d_model), BF16),
            pltpu.VMEM((tokens, d_model), BF16),
            pltpu.VMEM((tokens, d_model), BF16),
            pltpu.VMEM((tokens, d_model), F32),
            dma((7, 4)), dma((7, 4)), dma((7, 4)), dma((7, 4)), dma((6,)), dma((6,)),
            dma((2, N_FOUR)), dma((3, N_FOUR)), dma((2,)), dma((N_H,)), dma((N_PAIR,)), dma((N_PAIR,)),
            dma((4,)), dma((4,)), dma((4,)),
        ],
        compiler_params=pltpu.CompilerParams(collective_id=0, has_side_effects=True, vmem_limit_bytes=67000000),
        name="mlp_step",
    )(w1, w2, x, g)
    return deliver(outs[0], outs[1], outs[2])


N_PART = 8


def deliver(y, gup, gdown):
    def body(y_in, up_in, down_in, y_out, up_out, down_out, y_buf, up_buf, down_buf, sems_in, sems_out):
        srcs, dsts, bufs = (y_in, up_in, down_in), (y_out, up_out, down_out), (y_buf, up_buf, down_buf)
        moves = []
        for p in range(N_PART):
            for n in range(3):
                rows = srcs[n].shape[0] // N_PART
                part = pl.ds(p * rows, rows)
                moves.append((pltpu.make_async_copy(srcs[n].at[part, :], bufs[n].at[part, :], sems_in.at[n, p]),
                              pltpu.make_async_copy(bufs[n].at[part, :], dsts[n].at[part, :], sems_out.at[n, p])))
        for cp, _ in moves:
            cp.start()
        for cp_in, cp_out in moves:
            cp_in.wait()
            cp_out.start()
        for _, cp in moves:
            cp.wait()

    any_spec = pl.BlockSpec(memory_space=pl.ANY)
    arrays = (y, gup, gdown)
    return pl.pallas_call(
        body,
        out_shape=tuple(jax.ShapeDtypeStruct(a.shape, a.dtype) for a in arrays),
        in_specs=[any_spec] * 3,
        out_specs=(any_spec,) * 3,
        scratch_shapes=[pltpu.VMEM(a.shape, a.dtype) for a in arrays] +
        [pltpu.SemaphoreType.DMA((3, N_PART)), pltpu.SemaphoreType.DMA((3, N_PART))],
        compiler_params=pltpu.CompilerParams(vmem_limit_bytes=60000000),
        name="deliver",
    )(*arrays)


def solution(mesh):
    row_spec = P(None, 'fsdp', None)

    def per_device(w_up, w_down, tokens_in, cotangent):
        width = tokens_in.shape[-1]
        y, gup, gdown = fused_step(w_up[0], w_down[0], tokens_in.reshape(-1, width), cotangent.reshape(-1, width))
        return y.reshape(tokens_in.shape), gup[None], gdown[None]

    return jax.shard_map(per_device, mesh=mesh, in_specs=(row_spec,) * 4, out_specs=(row_spec,) * 3, check_vma=False)
```
